16 devices in a mesh: rep: 2 (over y, z), pool: 8 (over x, core).
Axes of the slice: x: 4, y: 2, z: 1, core: 2. Of those that a mesh axis runs over, the one named last changes fastest.
The devices are a block of a 4x4x8 slice.
Arguments:
- kv_pool: bfloat16 [3, 1024, 2, 32, 16, 128], P(None, ('rep', 'pool')), parts along dimension 1
- page_idx: int32 [8, 16, 8], P(None, ('rep', 'pool')), parts along dimension 1
- tok_hidden: bfloat16 [16, 64, 2048], P(('rep', 'pool')), parts along dimension 0
- attn_norm: bfloat16 [3, 2048], replicated
- w_query: bfloat16 [3, 2048, 2048], replicated
- w_key: bfloat16 [3, 2048, 2048], replicated
- w_value: bfloat16 [3, 2048, 2048], replicated
- w_out: bfloat16 [3, 2048, 2048], replicated
- mlp_norm: bfloat16 [3, 2048], replicated
- w_gate: bfloat16 [3, 2048, 5504], replicated
- w_up: bfloat16 [3, 2048, 5504], replicated
- w_down: bfloat16 [3, 5504, 2048], replicated
Outputs:
- output: bfloat16 [16, 64, 2048], P(('rep', 'pool')), parts along dimension 0
There are 2 independent parts. The reference program is written for one: setup_inputs(seed, part) draws one part's arguments, and reference() takes and returns one part's arrays. A program takes and returns all parts, laid end to end along the dimension named above; an argument that names none is the same for every part.
All inputs are finite; a program needn't handle non-finite values.
Results may differ from the reference program's by a relative error of at most 0.02.
Values are sent between devices in bfloat16 or wider.
A program may use at most 768 MiB of HBM per device.

```python
import math
import jax
import jax.numpy as jnp
from jax import lax

GROUP = 8
LAYERS = 3
TOKENS = 64
PAGE_LEN = 32
SLOTS = 8
POOL_PAGES = 64
HIDDEN = 2048
NUM_HEADS = 16
HEAD_DIM = 128
FF_DIM = 5504
ROPE_BASE = 10000

PREFIX = GROUP * SLOTS * PAGE_LEN
ATTN_WIDTH = NUM_HEADS * HEAD_DIM


def setup_inputs(seed: int = 0, part: int = 0) -> dict:
    part_key = jax.random.fold_in(jax.random.key(seed), part)
    pool_key, idx_key, hid_key = jax.random.split(part_key, 3)
    weight_keys = jax.random.split(jax.random.key(seed + 1), 9)
    kv_pool = jax.random.normal(pool_key, (LAYERS, GROUP * POOL_PAGES, 2, PAGE_LEN, NUM_HEADS, HEAD_DIM), jnp.float32).astype(jnp.bfloat16)
    owner_keys = jax.random.split(idx_key, GROUP)
    page_perm = jax.vmap(lambda owner_key: jax.random.permutation(owner_key, POOL_PAGES))(owner_keys)
    chosen = page_perm[:, : GROUP * SLOTS].reshape(GROUP, GROUP, SLOTS)
    page_idx = jnp.transpose(chosen, (1, 0, 2)).astype(jnp.int32)
    tok_hidden = jax.random.normal(hid_key, (GROUP, TOKENS, HIDDEN), jnp.float32).astype(jnp.bfloat16)

    def make_weight(key, shape, fan_in, gain):
        return (jax.random.normal(key, shape, jnp.float32) * (gain / math.sqrt(fan_in))).astype(jnp.bfloat16)

    def make_gain(key):
        return (1.0 + 0.3 * jax.random.normal(key, (LAYERS, HIDDEN), jnp.float32)).astype(jnp.bfloat16)

    return {
        'kv_pool': kv_pool,
        'page_idx': page_idx,
        'tok_hidden': tok_hidden,
        'attn_norm': make_gain(weight_keys[0]),
        'w_query': make_weight(weight_keys[1], (LAYERS, HIDDEN, ATTN_WIDTH), HIDDEN, 2.5),
        'w_key': make_weight(weight_keys[2], (LAYERS, HIDDEN, ATTN_WIDTH), HIDDEN, 1.0),
        'w_value': make_weight(weight_keys[3], (LAYERS, HIDDEN, ATTN_WIDTH), HIDDEN, 1.0),
        'w_out': make_weight(weight_keys[4], (LAYERS, ATTN_WIDTH, HIDDEN), ATTN_WIDTH, 1.0),
        'mlp_norm': make_gain(weight_keys[5]),
        'w_gate': make_weight(weight_keys[6], (LAYERS, HIDDEN, FF_DIM), HIDDEN, 1.0),
        'w_up': make_weight(weight_keys[7], (LAYERS, HIDDEN, FF_DIM), HIDDEN, 1.0),
        'w_down': make_weight(weight_keys[8], (LAYERS, FF_DIM, HIDDEN), FF_DIM, 1.0),
    }


def rms_norm(vals, gain):
    vals_f = vals.astype(jnp.float32)
    inv_rms = lax.rsqrt(jnp.mean(vals_f * vals_f, axis=-1, keepdims=True) + 1e-6)
    return (vals_f * inv_rms * gain.astype(jnp.float32)).astype(jnp.bfloat16)


def rope_tables():
    positions = (PREFIX + jnp.arange(TOKENS)).astype(jnp.float32)
    exponent = jnp.arange(HEAD_DIM // 2).astype(jnp.float32) * (-2.0 / HEAD_DIM)
    inv_freq = jnp.power(float(ROPE_BASE), exponent)
    angles = positions[:, None] * inv_freq[None, :]
    return jnp.cos(angles)[:, None, :], jnp.sin(angles)[:, None, :]


def apply_rope(proj, cosine, sine):
    half = HEAD_DIM // 2
    first = proj[..., :half]
    second = proj[..., half:]
    return jnp.concatenate([first * cosine - second * sine, second * cosine + first * sine], axis=-1)


def reference(kv_pool, page_idx, tok_hidden, attn_norm, w_query, w_key, w_value, w_out, mlp_norm, w_gate, w_up, w_down):
    cosine, sine = rope_tables()
    owner_base = (jnp.arange(GROUP) * POOL_PAGES)[:, None]
    causal = jnp.arange(TOKENS)[None, :] <= jnp.arange(TOKENS)[:, None]
    visible = jnp.concatenate([jnp.full((TOKENS, PREFIX), True), causal], axis=1)
    scale = 1.0 / math.sqrt(HEAD_DIM)
    layer_stack = (kv_pool, attn_norm, w_query, w_key, w_value, w_out, mlp_norm, w_gate, w_up, w_down)
    head_shape = (TOKENS, NUM_HEADS, HEAD_DIM)

    def one_request(request_in):
        tok_rows, page_rows = request_in
        flat_pages = (page_rows + owner_base).reshape(GROUP * SLOTS)

        def layer_step(hidden, layer_in):
            layer_pool, gain_attn, q_weight, k_weight, v_weight, o_weight, gain_mlp, gate_weight, up_weight, down_weight = layer_in
            fetched = layer_pool[flat_pages]
            key_pre = fetched[:, 0].reshape(PREFIX, NUM_HEADS, HEAD_DIM)
            val_pre = fetched[:, 1].reshape(PREFIX, NUM_HEADS, HEAD_DIM)
            normed = rms_norm(hidden, gain_attn)
            query = apply_rope(jnp.dot(normed, q_weight, preferred_element_type=jnp.float32).reshape(head_shape), cosine, sine).astype(jnp.bfloat16)
            key_new = apply_rope(jnp.dot(normed, k_weight, preferred_element_type=jnp.float32).reshape(head_shape), cosine, sine).astype(jnp.bfloat16)
            val_new = jnp.dot(normed, v_weight, preferred_element_type=jnp.float32).astype(jnp.bfloat16).reshape(head_shape)
            keys_all = jnp.concatenate([key_pre, key_new], axis=0)
            vals_all = jnp.concatenate([val_pre, val_new], axis=0)
            scores = jnp.einsum('thd,nhd->htn', query.astype(jnp.float32), keys_all.astype(jnp.float32)) * scale
            scores = jnp.where(visible[None, :, :], scores, -1e30)
            attn_prob = jax.nn.softmax(scores, axis=-1).astype(jnp.bfloat16)
            mixed = jnp.einsum('htn,nhd->thd', attn_prob.astype(jnp.float32), vals_all.astype(jnp.float32))
            attn_out = mixed.astype(jnp.bfloat16).reshape(TOKENS, ATTN_WIDTH)
            hidden = (hidden.astype(jnp.float32) + jnp.dot(attn_out, o_weight, preferred_element_type=jnp.float32)).astype(jnp.bfloat16)
            normed_mlp = rms_norm(hidden, gain_mlp)
            gate = jnp.dot(normed_mlp, gate_weight, preferred_element_type=jnp.float32)
            upper = jnp.dot(normed_mlp, up_weight, preferred_element_type=jnp.float32)
            inner = (jax.nn.silu(gate) * upper).astype(jnp.bfloat16)
            hidden = (hidden.astype(jnp.float32) + jnp.dot(inner, down_weight, preferred_element_type=jnp.float32)).astype(jnp.bfloat16)
            return hidden, None

        out_rows, _ = lax.scan(layer_step, tok_rows, layer_stack)
        return out_rows

    return lax.map(one_request, (tok_hidden, page_idx))
```

```python
import functools
import math
import numpy as np
import jax
import jax.numpy as jnp
from jax import lax
from jax.experimental import pallas as pl
from jax.experimental.pallas import tpu as pltpu
from jax.sharding import PartitionSpec as P

NORM_EPS = 1e-6
ROPE_BASE = 10000.0
LOG2E = 1.4426950408889634
NEG = -1e30
MESH = pl.DeviceIdType.MESH
BF = jnp.bfloat16
F32 = jnp.float32

CORES = 2
CHIPS = 4
COL = 256
PAIRS = 6
STAGE = 8
PITCH = 36
OUT_COL = 512


def rope_tables(offset, tokens, head_dim):
    positions = (offset + np.arange(tokens)).astype(np.float32)
    exponent = np.arange(head_dim // 2).astype(np.float32) * np.float32(-2.0 / head_dim)
    inv_freq = np.power(np.float32(ROPE_BASE), exponent).astype(np.float32)
    angles = (positions[:, None] * inv_freq[None, :]).astype(np.float32)
    cosine, sine = np.cos(angles), np.sin(angles)
    return np.concatenate([cosine, cosine], 1), np.concatenate([-sine, sine], 1)


def kernel(cfg, idx, hid, cos, sin, gain_a, gain_m, kv, wq, wk, wv, wo, wg, wu, wd, out,
           x, h, att, inner, q, k_new, v_new, pages, stage, unpack,
           p_loc, p_send, p_recv, s_loc, s_send, s_recv, n_o, n_s,
           f_o, f_s, fin_o, fin_s, px_send, px_recv, ring, wo_buf, wd_buf,
           ring_sem, wo_sem, wd_sem, stage_sem,
           x_sem, qp_sem, qr_sem, ql_sem, po_sem, ro_sem, lo_sem, px_sem):
    layers, tokens, dim, heads, hd, ff, n_pages, slots = cfg
    group = CORES * CHIPS
    half = heads // CORES
    part = half // 2
    rows = CORES * tokens
    width = half * hd
    ff_cols = wd_buf.shape[1]
    ff_chunks = ff_cols // COL
    overlap = CORES * ff_cols - ff
    me = lax.axis_index("pool")
    chip = lax.div(me, CORES)
    core = lax.rem(me, CORES)
    partner = me + 1 - 2 * core
    right = lax.rem(me + CORES, group)
    left = lax.rem(me + group - CORES, group)
    c_right = lax.rem(chip + 1, CHIPS)
    c_left = lax.rem(chip + CHIPS - 1, CHIPS)
    c_far = lax.rem(chip + 2, CHIPS)
    other = 1 - core
    OWN, RIGHT, LEFT, FAR = 0, 1, 2, 3
    chip_of = {OWN: chip, RIGHT: c_right, LEFT: c_left, FAR: c_far}
    score_scale = LOG2E / math.sqrt(hd)

    def remote(src, dst, sem, dev):
        return pltpu.make_async_remote_copy(src_ref=src, dst_ref=dst, send_sem=sem.at[0], recv_sem=sem.at[1],
                                            device_id={"pool": dev}, device_id_type=MESH)

    def qkv_copy(l, t, w, sub):
        base = lax.rem(t, 2) * 2 * COL + sub * COL
        col = pl.multiple_of(core * width + base, COL)
        slot = 2 * t + sub
        return pltpu.make_async_copy(w.at[l, :, pl.ds(col, COL)], ring.at[slot], ring_sem.at[slot])

    def start_qkv(l, t):
        for n, w in enumerate((wq, wk, wv)):
            @pl.when(lax.div(t, 2) == n)
            def _(w=w):
                for sub in range(2):
                    qkv_copy(l, t, w, sub).start()

    def gu_copy(l, j, sub):
        col = pl.multiple_of(core * (ff - ff_cols) + j * COL, 128)
        slot = 2 * lax.rem(j, PAIRS) + sub
        return pltpu.make_async_copy((wg, wu)[sub].at[l, :, pl.ds(col, COL)], ring.at[slot], ring_sem.at[slot])

    def wo_copy(l, n):
        return pltpu.make_async_copy(wo.at[l, pl.ds(pl.multiple_of(core * width, width), width), pl.ds(pl.multiple_of(n * OUT_COL, OUT_COL), OUT_COL)],
                                     wo_buf.at[n], wo_sem.at[n])

    def wd_copy(l, n):
        row = pl.multiple_of(core * (ff - ff_cols), 128)
        return pltpu.make_async_copy(wd.at[l, pl.ds(row, ff_cols), pl.ds(pl.multiple_of(n * COL, COL), COL)],
                                     wd_buf.at[n], wd_sem.at[n])

    page_len = kv.shape[3]

    def page_copy(l, p):
        s = lax.rem(p, STAGE)
        return pltpu.make_async_copy(kv.at[l, p], stage.at[s], stage_sem.at[s])

    def turn_pages(l, lo, hi):
        def body(p, carry):
            page_copy(l, p).wait()
            s = lax.rem(p, STAGE)
            for b in range(2):
                for r in range(page_len):
                    unpack[b, pl.ds(r, heads, stride=PITCH), :] = stage[s, b, r].astype(F32)
            for b in range(2):
                for i in range(heads):
                    pages[p, b, i] = unpack[b, pl.ds(i * PITCH, page_len), :].astype(BF)
            nxt = p + STAGE

            @pl.when(nxt < n_pages)
            def _():
                page_copy(l, nxt).start()

            @pl.when((nxt >= n_pages) & (l + 1 < layers))
            def _():
                page_copy(l + 1, nxt - n_pages).start()
            return carry
        lax.fori_loop(lo, hi, body, 0)

    def q_right(n):
        src = (q.at[chip, core, 0], q.at[chip, core, 1], q.at[c_left, core, 0])[n]
        return remote(src, src, qr_sem.at[n], right)

    def q_left(n):
        src = (q.at[chip, core, 1], q.at[chip, core, 0], q.at[c_right, core, 1])[n]
        return remote(src, src, ql_sem.at[n], left)

    def q_part(n):
        src = (q.at[chip, core, 0], q.at[chip, core, 1], q.at[c_left, core, 0], q.at[c_left, core, 1],
               q.at[c_right, core, 0], q.at[c_right, core, 1], q.at[c_far, core, 0], q.at[c_far, core, 1])[n]
        return remote(src, src, qp_sem.at[n], partner)

    def o_part(d):
        return (remote(p_send.at[d], p_recv.at[d], po_sem.at[d, 0], partner),
                remote(s_send.at[d], s_recv.at[d], po_sem.at[d, 1], partner))

    def o_right(n):
        d, j, dst_o, dst_s = ((RIGHT, 1, fin_o.at[0, 1], fin_s.at[0, 1]), (FAR, 0, f_o.at[0], f_s.at[0]),
                              (RIGHT, 0, fin_o.at[0, 0], fin_s.at[0, 0]))[n]
        return (remote(p_loc.at[d, j], dst_o, ro_sem.at[n, 0], right), remote(s_loc.at[d, j], dst_s, ro_sem.at[n, 1], right))

    def o_left(n):
        d, j, dst_o, dst_s = ((LEFT, 0, fin_o.at[1, 0], fin_s.at[1, 0]), (FAR, 1, f_o.at[1], f_s.at[1]),
                              (LEFT, 1, fin_o.at[1, 1], fin_s.at[1, 1]))[n]
        return (remote(p_loc.at[d, j], dst_o, lo_sem.at[n, 0], left), remote(s_loc.at[d, j], dst_s, lo_sem.at[n, 1], left))

    def px_copy(which, n):
        return remote(px_send.at[n], px_recv.at[which, n], px_sem.at[which, n], partner)

    def start(copies):
        for cp in copies:
            cp.start()

    def wait_recv(copies):
        for cp in copies:
            cp.wait_recv()

    def wait_send(copies):
        for cp in copies:
            cp.wait_send()

    lane = lax.broadcasted_iota(jnp.int32, (tokens, 128), 1)

    def softmax_part(qv, kk, vv, mask=None):
        s = lax.dot_general(qv, kk, (((1,), (1,)), ((), ())), preferred_element_type=F32) * score_scale
        if mask is not None:
            s = jnp.where(mask, s, NEG)
        m = jnp.max(s, axis=1, keepdims=True)
        p = jnp.exp2(s - m)
        z = jnp.sum(p, axis=1, keepdims=True)
        return jnp.dot(p.astype(BF), vv, preferred_element_type=F32), m, z

    def attend_pages(d, hb, o_ref, s_ref):
        ca = chip_of[d]

        def body(t, carry):
            j = lax.div(t, 2)
            g = lax.rem(t, 2)
            where = [idx[(CORES * ca + j) * slots + s] for s in range(slots)]
            stats = s_ref[d, j]
            for ii in range(part):
                head = hb * half + g * part + ii
                kk = jnp.concatenate([pages[w, 0, head] for w in where], axis=0)
                vv = jnp.concatenate([pages[w, 1, head] for w in where], axis=0)
                o, m, z = softmax_part(q[ca, hb, g, ii, j], kk, vv)
                o_ref[d, j, g * part + ii] = o
                stats = jnp.where(lane == g * part + ii, m, jnp.where(lane == half + g * part + ii, z, stats))
            s_ref[d, j] = stats
            return carry
        lax.fori_loop(0, 2 * CORES, body, 0)

    def attend_new():
        row = lax.broadcasted_iota(jnp.int32, (tokens, tokens), 0)
        col = lax.broadcasted_iota(jnp.int32, (tokens, tokens), 1)
        mask = col <= row

        def body(j, carry):
            stats = n_s[j]
            for i in range(half):
                o, m, z = softmax_part(q[chip, core, i // part, i % part, j], k_new[i, j], v_new[i, j], mask)
                n_o[j, i] = o
                stats = jnp.where(lane == i, m, jnp.where(lane == half + i, z, stats))
            n_s[j] = stats
            return carry
        lax.fori_loop(0, CORES, body, 0)

    def merge(ao, a_s, bo, b_s):
        sa, sb = a_s[...], b_s[...]
        m = jnp.maximum(sa, sb)
        wa, wb = jnp.exp2(sa - m), jnp.exp2(sb - m)
        z = sa * pltpu.roll(wa, half, axis=1) + sb * pltpu.roll(wb, half, axis=1)
        a_s[...] = jnp.where(lane < half, m, jnp.where(lane < 2 * half, z, 0.0))
        for i in range(half):
            ao[i] = ao[i] * wa[:, i:i + 1] + bo[i] * wb[:, i:i + 1]

    def merge_pair(d, j):
        merge(p_loc.at[d, j], s_loc.at[d, j], p_recv.at[d, j], s_recv.at[d, j])

    def norm_rows(v, gain):
        inv = lax.rsqrt(jnp.mean(v * v, axis=-1, keepdims=True) + NORM_EPS)
        return (v * inv * gain).astype(BF)

    ROWS = 16

    def norm_only(gain):
        def body(b, carry):
            r = pl.ds(pl.multiple_of(b * ROWS, ROWS), ROWS)
            h[r, :] = norm_rows(x[r, :].astype(F32), gain)
            return carry
        lax.fori_loop(0, rows // ROWS, body, 0)

    def add_norm(which, gain):
        n_col = dim // OUT_COL
        for n in range(n_col):
            px_copy(which, n).wait()

        def body(b, carry):
            r = pl.ds(pl.multiple_of(b * ROWS, ROWS), ROWS)
            total = jnp.concatenate([px_send[n, r, :] + px_recv[which, n, r, :] for n in range(n_col)], axis=1)
            xv = (x[r, :].astype(F32) + total).astype(BF)
            x[r, :] = xv
            h[r, :] = norm_rows(xv.astype(F32), gain)
            return carry
        lax.fori_loop(0, rows // ROWS, body, 0)

    def dot(a, b):
        return jnp.dot(a, b, preferred_element_type=F32)

    def qkv_pair(l, t):
        w = (wq, wk, wv)[t // 2]
        for sub in range(2):
            qkv_copy(l, t, w, sub).wait()
        hv = h[...]
        for sub in range(2):
            res = dot(hv, ring[2 * t + sub])
            for e in range(COL // hd):
                v = res[:, e * hd:(e + 1) * hd]
                if t < 4:
                    v = v * cos[...] + pltpu.roll(v, hd // 2, axis=1) * sin[...]
                v = v.astype(BF)
                i = (t % 2) * part + sub * (COL // hd) + e
                for j in range(CORES):
                    vj = v[j * tokens:(j + 1) * tokens]
                    if t < 2:
                        q[chip, core, i // part, i % part, j] = vj
                    elif t < 4:
                        k_new[i, j] = vj
                    else:
                        v_new[i, j] = vj
        for sub in range(2):
            gu_copy(l, t, sub).start()

    barrier = pltpu.get_barrier_semaphore()
    for dev in (partner, left, right):
        pl.semaphore_signal(barrier, inc=1, device_id={"pool": dev}, device_id_type=MESH)
    for t in range(PAIRS):
        start_qkv(0, t)
    for p in range(STAGE):
        page_copy(0, p).start()
    s_loc[...] = jnp.zeros_like(s_loc)
    s_send[...] = jnp.zeros_like(s_send)
    n_s[...] = jnp.zeros_like(n_s)
    own_rows = pl.ds(pl.multiple_of(core * tokens, tokens), tokens)
    x[own_rows, :] = hid[...]
    pl.semaphore_wait(barrier, 3)
    x_copy = remote(hid, x.at[own_rows], x_sem, partner)
    x_copy.start()
    for n in range(dim // OUT_COL):
        wo_copy(0, n).start()
    for n in range(dim // COL):
        wd_copy(0, n).start()
    turn_pages(0, 0, n_pages)
    x_copy.wait()
    norm_only(gain_a[0])

    def layer(l, carry):
        for t in range(2):
            qkv_pair(l, t)
        for n in range(2):
            q_right(n).start()
            q_left(n).start()
        for n in range(2):
            q_part(n).start()
        for t in range(2, 6):
            qkv_pair(l, t)
        attend_new()
        attend_pages(OWN, core, p_loc, s_loc)

        q_right(0).wait_recv()
        q_right(2).start()
        q_part(2).start()
        q_left(0).wait_recv()
        q_left(2).start()
        q_part(5).start()

        q_part(0).wait_recv()
        q_part(1).wait_recv()
        attend_pages(OWN, other, p_send, s_send)
        start(o_part(OWN))

        q_right(1).wait_recv()
        q_part(3).start()
        q_left(1).wait_recv()
        q_part(4).start()
        attend_pages(LEFT, core, p_loc, s_loc)
        attend_pages(RIGHT, core, p_loc, s_loc)
        q_part(2).wait_recv()
        q_part(3).wait_recv()
        attend_pages(LEFT, other, p_send, s_send)
        start(o_part(LEFT))
        q_right(2).wait_recv()
        q_part(6).start()
        q_left(2).wait_recv()
        q_part(7).start()
        q_part(4).wait_recv()
        q_part(5).wait_recv()
        attend_pages(RIGHT, other, p_send, s_send)
        start(o_part(RIGHT))

        wait_recv(o_part(LEFT))
        merge_pair(LEFT, 0)
        start(o_left(0))
        wait_recv(o_part(RIGHT))
        merge_pair(RIGHT, 1)
        start(o_right(0))

        q_part(6).wait_recv()
        q_part(7).wait_recv()
        attend_pages(FAR, other, p_send, s_send)
        start(o_part(FAR))
        attend_pages(FAR, core, p_loc, s_loc)
        wait_recv(o_part(FAR))
        merge_pair(FAR, 0)
        start(o_right(1))
        merge_pair(FAR, 1)
        start(o_left(1))
        merge_pair(RIGHT, 0)
        merge_pair(LEFT, 1)
        wait_recv(o_part(OWN))
        for j in range(CORES):
            merge_pair(OWN, j)
            merge(p_loc.at[OWN, j], s_loc.at[OWN, j], n_o.at[j], n_s.at[j])
        for n in range(8):
            q_part(n).wait_send()
        for n in range(3):
            q_right(n).wait_send()
            q_left(n).wait_send()
        for d in range(4):
            wait_send(o_part(d))

        @pl.when(l + 1 < layers)
        def _():
            turn_pages(l + 1, 0, n_pages // 2)

        wait_recv(o_right(1))
        merge(p_loc.at[RIGHT, 0], s_loc.at[RIGHT, 0], f_o.at[0], f_s.at[0])
        start(o_right(2))
        wait_recv(o_left(1))
        merge(p_loc.at[LEFT, 1], s_loc.at[LEFT, 1], f_o.at[1], f_s.at[1])
        start(o_left(2))

        @pl.when(l + 1 < layers)
        def _():
            turn_pages(l + 1, n_pages // 2, n_pages)

        wait_recv(o_right(0))
        merge(p_loc.at[OWN, 1], s_loc.at[OWN, 1], fin_o.at[0, 1], fin_s.at[0, 1])
        wait_recv(o_left(0))
        merge(p_loc.at[OWN, 0], s_loc.at[OWN, 0], fin_o.at[1, 0], fin_s.at[1, 0])
        wait_recv(o_right(2))
        merge(p_loc.at[OWN, 0], s_loc.at[OWN, 0], fin_o.at[0, 0], fin_s.at[0, 0])
        wait_recv(o_left(2))
        merge(p_loc.at[OWN, 1], s_loc.at[OWN, 1], fin_o.at[1, 1], fin_s.at[1, 1])
        for n in range(3):
            wait_send(o_right(n))
            wait_send(o_left(n))
        for j in range(CORES):
            inv = 1.0 / s_loc[OWN, j]
            for i in range(half):
                att[j * tokens:(j + 1) * tokens, i * hd:(i + 1) * hd] = (p_loc[OWN, j, i] * inv[:, half + i:half + i + 1]).astype(BF)

        def out_body(n, carry):
            wo_copy(l, n).wait()
            px_send[n] = dot(att[...], wo_buf[n])
            px_copy(0, n).start()

            @pl.when(l + 1 < layers)
            def _():
                wo_copy(l + 1, n).start()
            return carry
        lax.fori_loop(0, dim // OUT_COL, out_body, 0)
        add_norm(0, gain_m[l])

        def gu_body(j, carry):
            for sub in range(2):
                gu_copy(l, j, sub).wait()
            sp = lax.rem(j, PAIRS)
            hv = h[...]
            gate = dot(hv, ring[2 * sp])
            upper = dot(hv, ring[2 * sp + 1])
            val = gate / (1.0 + jnp.exp(-gate)) * upper
            col = lax.broadcasted_iota(jnp.int32, (rows, COL), 1) + j * COL
            val = jnp.where(col >= core * overlap, val, 0.0)
            inner[:, pl.ds(pl.multiple_of(j * COL, COL), COL)] = val.astype(BF)

            @pl.when(j + PAIRS < ff_chunks)
            def _():
                for sub in range(2):
                    gu_copy(l, j + PAIRS, sub).start()

            @pl.when((j + PAIRS >= ff_chunks) & (l + 1 < layers))
            def _():
                start_qkv(l + 1, sp)
            return carry
        lax.fori_loop(0, ff_chunks, gu_body, 0)

        def down_body(n, carry):
            iv = inner[...]
            for sub in range(OUT_COL // COL):
                wd_copy(l, 2 * n + sub).wait()
            for sub in range(OUT_COL // COL):
                px_send[n, :, sub * COL:(sub + 1) * COL] = dot(iv, wd_buf[2 * n + sub])
            px_copy(1, n).start()

            @pl.when(l + 1 < layers)
            def _():
                for sub in range(OUT_COL // COL):
                    wd_copy(l + 1, 2 * n + sub).start()
            return carry
        lax.fori_loop(0, dim // OUT_COL, down_body, 0)
        add_norm(1, gain_a[lax.rem(l + 1, layers)])
        return carry
    lax.fori_loop(0, layers, layer, 0)
    out[...] = x[own_rows, :]


def solution(mesh):
    group = mesh.shape["pool"]

    def local_program(kv, idx, hid, attn_norm, w_query, w_key, w_value, w_out, mlp_norm, w_gate, w_up, w_down):
        layers, n_pages, _, page_len, heads, hd = kv.shape
        slots = idx.shape[2]
        _, tokens, dim = hid.shape
        ff = w_gate.shape[2]
        half, rows = heads // CORES, CORES * tokens
        ff_cols = -(-ff // (CORES * COL)) * COL
        cosine, sine = rope_tables(group * slots * page_len, tokens, hd)
        cos2 = jnp.asarray(np.tile(cosine, (CORES, 1)))
        sin2 = jnp.asarray(np.tile(sine, (CORES, 1)))
        cfg = (layers, tokens, dim, heads, hd, ff, n_pages, slots)
        vmem = pl.BlockSpec(memory_space=pltpu.VMEM)
        hbm = pl.BlockSpec(memory_space=pl.ANY)
        smem = pl.BlockSpec(memory_space=pltpu.SMEM)
        dma = pltpu.SemaphoreType.DMA
        o_block = (half, tokens, hd)
        s_block = (tokens, 128)
        n_out = dim // OUT_COL
        scratch = [
            pltpu.VMEM((rows, dim), BF), pltpu.VMEM((rows, dim), BF), pltpu.VMEM((rows, half * hd), BF), pltpu.VMEM((rows, ff_cols), BF),
            pltpu.VMEM((CHIPS, CORES, 2, half // 2, CORES, tokens, hd), BF),
            pltpu.VMEM((half, CORES, tokens, hd), BF), pltpu.VMEM((half, CORES, tokens, hd), BF),
            pltpu.VMEM((n_pages, 2, heads, page_len, hd), BF),
            pltpu.VMEM((STAGE, 2, page_len, heads, hd), BF),
            pltpu.VMEM((2, heads * PITCH, hd), F32),
            pltpu.VMEM((4, CORES) + o_block, F32), pltpu.VMEM((4, CORES) + o_block, F32), pltpu.VMEM((4, CORES) + o_block, F32),
            pltpu.VMEM((4, CORES) + s_block, F32), pltpu.VMEM((4, CORES) + s_block, F32), pltpu.VMEM((4, CORES) + s_block, F32),
            pltpu.VMEM((CORES,) + o_block, F32), pltpu.VMEM((CORES,) + s_block, F32),
            pltpu.VMEM((2,) + o_block, F32), pltpu.VMEM((2,) + s_block, F32),
            pltpu.VMEM((2, CORES) + o_block, F32), pltpu.VMEM((2, CORES) + s_block, F32),
            pltpu.VMEM((n_out, rows, OUT_COL), F32), pltpu.VMEM((2, n_out, rows, OUT_COL), F32),
            pltpu.VMEM((2 * PAIRS, dim, COL), BF), pltpu.VMEM((n_out, half * hd, OUT_COL), BF), pltpu.VMEM((dim // COL, ff_cols, COL), BF),
            dma((2 * PAIRS,)), dma((n_out,)), dma((dim // COL,)), dma((STAGE,)),
            dma((2,)), dma((8, 2)), dma((3, 2)), dma((3, 2)), dma((4, 2, 2)), dma((3, 2, 2)), dma((3, 2, 2)), dma((2, n_out, 2)),
        ]
        result = pl.pallas_call(
            functools.partial(kernel, cfg),
            out_shape=jax.ShapeDtypeStruct((tokens, dim), BF),
            in_specs=[smem] + [vmem] * 5 + [hbm] * 8,
            out_specs=vmem,
            scratch_shapes=scratch,
            compiler_params=pltpu.CompilerParams(collective_id=0, has_side_effects=True, vmem_limit_bytes=67043328),
            name="decoder",
        )(idx.reshape(-1), hid[0], cos2, sin2, attn_norm.astype(F32)[:, None, :], mlp_norm.astype(F32)[:, None, :],
          kv, w_query, w_key, w_value, w_out, w_gate, w_up, w_down)
        return result[None]

    data_specs = (P(None, ("rep", "pool")), P(None, ("rep", "pool"), None), P(("rep", "pool")))
    return jax.shard_map(local_program, mesh=mesh, in_specs=data_specs + (P(),) * 9, out_specs=P(("rep", "pool")), check_vma=False)
```

```python
import functools
import math
import numpy as np
import jax
import jax.numpy as jnp
from jax import lax
from jax.experimental import pallas as pl
from jax.experimental.pallas import tpu as pltpu
from jax.sharding import PartitionSpec as P

NORM_EPS = 1e-6
ROPE_BASE = 10000.0
LOG2E = 1.4426950408889634
NEG = -1e30
MESH = pl.DeviceIdType.MESH
BF = jnp.bfloat16
F32 = jnp.float32

CORES = 2
CHIPS = 4
COL = 256
PAIRS = 6
STAGE = 8
PITCH = 36
OUT_COL = 512


def rope_tables(offset, tokens, head_dim):
    positions = (offset + np.arange(tokens)).astype(np.float32)
    exponent = np.arange(head_dim // 2).astype(np.float32) * np.float32(-2.0 / head_dim)
    inv_freq = np.power(np.float32(ROPE_BASE), exponent).astype(np.float32)
    angles = (positions[:, None] * inv_freq[None, :]).astype(np.float32)
    cosine, sine = np.cos(angles), np.sin(angles)
    return np.concatenate([cosine, cosine], 1), np.concatenate([-sine, sine], 1)


def kernel(cfg, idx, hid, cos, sin, gain_a, gain_m, kv, wq, wk, wv, wo, wg, wu, wd, out,
           x, h, att, inner, q, k_new, v_new, pages, stage, unpack,
           p_loc, p_send, p_recv, s_loc, s_send, s_recv, n_o, n_s,
           f_o, f_s, fin_o, fin_s, px_recv, raw, ring, wo_buf, wd_buf,
           ring_sem, wo_sem, wd_sem, stage_sem,
           x_sem, qp_sem, qr_sem, ql_sem, po_sem, ro_sem, lo_sem, px_sem):
    layers, tokens, dim, heads, hd, ff, n_pages, slots = cfg
    group = CORES * CHIPS
    half = heads // CORES
    part = half // 2
    rows = CORES * tokens
    width = half * hd
    ff_cols = wd_buf.shape[1]
    ff_chunks = ff_cols // COL
    overlap = CORES * ff_cols - ff
    me = lax.axis_index("pool")
    chip = lax.div(me, CORES)
    core = lax.rem(me, CORES)
    partner = me + 1 - 2 * core
    right = lax.rem(me + CORES, group)
    left = lax.rem(me + group - CORES, group)
    c_right = lax.rem(chip + 1, CHIPS)
    c_left = lax.rem(chip + CHIPS - 1, CHIPS)
    c_far = lax.rem(chip + 2, CHIPS)
    other = 1 - core
    OWN, RIGHT, LEFT, FAR = 0, 1, 2, 3
    chip_of = {OWN: chip, RIGHT: c_right, LEFT: c_left, FAR: c_far}
    score_scale = LOG2E / math.sqrt(hd)

    def remote(src, dst, sem, dev):
        return pltpu.make_async_remote_copy(src_ref=src, dst_ref=dst, send_sem=sem.at[0], recv_sem=sem.at[1],
                                            device_id={"pool": dev}, device_id_type=MESH)

    def qkv_copy(l, t, w, sub):
        base = lax.rem(t, 2) * 2 * COL + sub * COL
        col = pl.multiple_of(core * width + base, COL)
        slot = 2 * t + sub
        return pltpu.make_async_copy(w.at[l, :, pl.ds(col, COL)], ring.at[slot], ring_sem.at[slot])

    def start_qkv(l, t):
        for n, w in enumerate((wq, wk, wv)):
            @pl.when(lax.div(t, 2) == n)
            def _(w=w):
                for sub in range(2):
                    qkv_copy(l, t, w, sub).start()

    def gu_copy(l, j, sub):
        col = pl.multiple_of(core * (ff - ff_cols) + j * COL, 128)
        slot = 2 * lax.rem(j, PAIRS) + sub
        return pltpu.make_async_copy((wg, wu)[sub].at[l, :, pl.ds(col, COL)], ring.at[slot], ring_sem.at[slot])

    def wo_copy(l, n):
        return pltpu.make_async_copy(wo.at[l, pl.ds(pl.multiple_of(core * width, width), width), pl.ds(pl.multiple_of(n * OUT_COL, OUT_COL), OUT_COL)],
                                     wo_buf.at[n], wo_sem.at[n])

    def wd_copy(l, n):
        row = pl.multiple_of(core * (ff - ff_cols), 128)
        return pltpu.make_async_copy(wd.at[l, pl.ds(row, ff_cols), pl.ds(pl.multiple_of(n * COL, COL), COL)],
                                     wd_buf.at[n], wd_sem.at[n])

    page_len = kv.shape[3]

    def page_copy(l, p):
        s = lax.rem(p, STAGE)
        return pltpu.make_async_copy(kv.at[l, p], stage.at[s], stage_sem.at[s])

    def turn_pages(l, lo, hi):
        def body(p, carry):
            page_copy(l, p).wait()
            s = lax.rem(p, STAGE)
            for b in range(2):
                for r in range(page_len):
                    unpack[b, pl.ds(r, heads, stride=PITCH), :] = stage[s, b, r].astype(F32)
            for b in range(2):
                for i in range(heads):
                    pages[p, b, i] = unpack[b, pl.ds(i * PITCH, page_len), :].astype(BF)
            nxt = p + STAGE

            @pl.when(nxt < n_pages)
            def _():
                page_copy(l, nxt).start()

            @pl.when((nxt >= n_pages) & (l + 1 < layers))
            def _():
                page_copy(l + 1, nxt - n_pages).start()
            return carry
        lax.fori_loop(lo, hi, body, 0)

    def q_right(n):
        src = (q.at[chip, core, 0], q.at[chip, core, 1], q.at[c_left, core, 0])[n]
        return remote(src, src, qr_sem.at[n], right)

    def q_left(n):
        src = (q.at[chip, core, 1], q.at[chip, core, 0], q.at[c_right, core, 1])[n]
        return remote(src, src, ql_sem.at[n], left)

    def q_part(n):
        src = (q.at[chip, core, 0], q.at[chip, core, 1], q.at[c_left, core, 0], q.at[c_left, core, 1],
               q.at[c_right, core, 0], q.at[c_right, core, 1], q.at[c_far, core, 0], q.at[c_far, core, 1])[n]
        return remote(src, src, qp_sem.at[n], partner)

    def o_part(d, j):
        return (remote(p_send.at[d, j], p_recv.at[d, j], po_sem.at[d, j, 0], partner),
                remote(s_send.at[d, j], s_recv.at[d, j], po_sem.at[d, j, 1], partner))

    def message(d, j, dst_o, dst_s, sem, dev):
        lo, hi = pl.ds(0, part), pl.ds(part, part)
        return (remote(s_loc.at[d, j], dst_s, sem.at[0], dev), remote(p_loc.at[d, j, lo], dst_o.at[lo], sem.at[1], dev),
                remote(p_loc.at[d, j, hi], dst_o.at[hi], sem.at[2], dev))

    def o_right(n):
        d, j, dst_o, dst_s = ((RIGHT, 1, fin_o.at[0, 1], fin_s.at[0, 1]), (FAR, 0, f_o.at[0], f_s.at[0]),
                              (RIGHT, 0, fin_o.at[0, 0], fin_s.at[0, 0]))[n]
        return message(d, j, dst_o, dst_s, ro_sem.at[n], right)

    def o_left(n):
        d, j, dst_o, dst_s = ((LEFT, 0, fin_o.at[1, 0], fin_s.at[1, 0]), (FAR, 1, f_o.at[1], f_s.at[1]),
                              (LEFT, 1, fin_o.at[1, 1], fin_s.at[1, 1]))[n]
        return message(d, j, dst_o, dst_s, lo_sem.at[n], left)

    def px_copy(which, n):
        return remote(p_send.at[n, :, pl.ds(0, OUT_COL // hd)], px_recv.at[which, n], px_sem.at[which, n], partner)

    def put_partial(n, first, v):
        for j in range(CORES):
            for c in range(v.shape[1] // hd):
                p_send[n, j, first + c] = v[j * tokens:(j + 1) * tokens, c * hd:(c + 1) * hd]

    def start(copies):
        for cp in copies:
            cp.start()

    def wait_recv(copies):
        for cp in copies:
            cp.wait_recv()

    def wait_send(copies):
        for cp in copies:
            cp.wait_send()

    lane = lax.broadcasted_iota(jnp.int32, (tokens, 128), 1)

    def attention(blocks, stats, mask=None):
        scores = [lax.dot_general(qv, kk(), (((1,), (1,)), ((), ())), preferred_element_type=F32) for _, qv, kk, _, _ in blocks]
        scores = [s * score_scale for s in scores]
        if mask is not None:
            scores = [jnp.where(mask, s, NEG) for s in scores]
        tops = [jnp.max(s, axis=1, keepdims=True) for s in scores]
        probs = [jnp.exp2(s - m) for s, m in zip(scores, tops)]
        sums = [jnp.sum(p, axis=1, keepdims=True) for p in probs]
        probs = [p.astype(BF) for p in probs]
        for (i, _, _, vv, store), p in zip(blocks, probs):
            store(jnp.dot(p, vv(), preferred_element_type=F32))
        for (i, _, _, _, _), m, z in zip(blocks, tops, sums):
            stats = jnp.where(lane == i, m, jnp.where(lane == half + i, z, stats))
        return stats

    def attend_pages(unit, hb, o_ref, s_ref):
        def body(t, carry):
            d, ca, j = unit(t)
            where = [idx[CORES * ca + j, 0, s] for s in range(slots)]
            blocks = []
            for i in range(half):
                def load(b, head=hb * half + i):
                    return jnp.concatenate([pages[w, b, head] for w in where], axis=0)

                def store(o, i=i):
                    o_ref[d, j, i] = o
                blocks.append((i, q[ca, hb, i // part, i % part, j], functools.partial(load, 0), functools.partial(load, 1), store))
            s_ref[d, j] = attention(blocks, s_ref[d, j])
            return carry
        lax.fori_loop(0, CORES, body, 0)

    def own_unit(t):
        return OWN, chip, t

    def far_unit(t):
        return FAR, c_far, t

    def near_first(t):
        return LEFT - t, lax.rem(chip + CHIPS - 1 + 2 * t, CHIPS), t

    def near_last(t):
        return LEFT - t, lax.rem(chip + CHIPS - 1 + 2 * t, CHIPS), 1 - t

    def attend_new():
        row = lax.broadcasted_iota(jnp.int32, (tokens, tokens), 0)
        col = lax.broadcasted_iota(jnp.int32, (tokens, tokens), 1)
        mask = col <= row

        def body(j, carry):
            blocks = []
            for i in range(half):
                def store(o, i=i):
                    n_o[j, i] = o
                blocks.append((i, q[chip, core, i // part, i % part, j], lambda i=i: k_new[i, j], lambda i=i: v_new[i, j], store))
            n_s[j] = attention(blocks, n_s[j], mask)
            return carry
        lax.fori_loop(0, CORES, body, 0)

    def weights(sa, sb):
        m = jnp.maximum(sa, sb)
        wa, wb = jnp.exp2(sa - m), jnp.exp2(sb - m)
        z = sa * pltpu.roll(wa, half, axis=1) + sb * pltpu.roll(wb, half, axis=1)
        return wa, wb, jnp.where(lane < half, m, jnp.where(lane < 2 * half, z, 0.0))

    def blend(ao, bo, wa, wb, i):
        return ao[i] * wa[:, i:i + 1] + bo[i] * wb[:, i:i + 1]

    def merge(ao, a_s, bo, b_s):
        wa, wb, a_s[...] = weights(a_s[...], b_s[...])
        for i in range(half):
            ao[i] = blend(ao, bo, wa, wb, i)

    def merge_pair(d, j):
        wait_recv(o_part(d, j))
        merge(p_loc.at[d, j], s_loc.at[d, j], p_recv.at[d, j], s_recv.at[d, j])

    def relay(copies, side, d, j, onward):
        ao, a_s, bo = p_loc.at[d, j], s_loc.at[d, j], f_o.at[side]
        wait_recv(copies[:2])
        wa, wb, a_s[...] = weights(a_s[...], f_s[side])
        for i in range(part):
            ao[i] = blend(ao, bo, wa, wb, i)
        start(onward[:2])
        wait_recv(copies[2:])
        for i in range(part, half):
            ao[i] = blend(ao, bo, wa, wb, i)
        start(onward[2:])

    def finish(copies, side, j):
        ao, bo = p_loc.at[OWN, j], fin_o.at[side, j]
        wait_recv(copies[:2])
        wa, wb, st = weights(s_loc[OWN, j], fin_s[side, j])
        inv = 1.0 / st
        for i in range(half):
            if i == part:
                wait_recv(copies[2:])
            o = blend(ao, bo, wa, wb, i) * inv[:, half + i:half + i + 1]
            att[j * tokens:(j + 1) * tokens, i * hd:(i + 1) * hd] = o.astype(BF)

    ROWS = 16
    n_col = dim // OUT_COL

    def normalise(squares, gain):
        inv = lax.rsqrt(jnp.sum(squares, axis=1, keepdims=True) * (1.0 / dim) + NORM_EPS)
        for r in range(0, rows, ROWS):
            h[r:r + ROWS, :] = (x[r:r + ROWS, :].astype(F32) * inv[r:r + ROWS] * gain).astype(BF)

    def square_tiles(v):
        v = v * v
        return sum(v[:, c:c + 128] for c in range(0, v.shape[1], 128))

    def gain_row(ref, l):
        g = ref[0:1, :].astype(F32)
        for n in range(1, layers):
            g = jnp.where(l == n, ref[n:n + 1, :].astype(F32), g)
        return g

    def norm_only(gain):
        normalise(square_tiles(x[...].astype(F32)), gain)

    def add_norm(which, gain):
        squares = jnp.zeros((rows, 128), F32)
        for n in range(n_col):
            px_copy(which, n).wait()
            for c in range(OUT_COL // hd):
                cols = slice(n * OUT_COL + c * hd, n * OUT_COL + (c + 1) * hd)
                total = jnp.concatenate([p_send[n, j, c] + px_recv[which, n, j, c] for j in range(CORES)], axis=0)
                xv = (x[:, cols].astype(F32) + total).astype(BF)
                x[:, cols] = xv
                xv = xv.astype(F32)
                squares = squares + xv * xv
        normalise(squares, gain)

    def dot(a, b):
        return jnp.dot(a, b, preferred_element_type=F32)

    def qkv_pair(l, t):
        w = (wq, wk, wv)[t // 2]
        for sub in range(2):
            qkv_copy(l, t, w, sub).wait()
        hv = h[...]
        for sub in range(2):
            res = dot(hv, ring[2 * t + sub])
            for e in range(COL // hd):
                v = res[:, e * hd:(e + 1) * hd]
                if t < 4:
                    v = v * cos[...] + pltpu.roll(v, hd // 2, axis=1) * sin[...]
                v = v.astype(BF)
                i = (t % 2) * part + sub * (COL // hd) + e
                for j in range(CORES):
                    vj = v[j * tokens:(j + 1) * tokens]
                    if t < 2:
                        q[chip, core, i // part, i % part, j] = vj
                    elif t < 4:
                        k_new[i, j] = vj
                    else:
                        v_new[i, j] = vj
    barrier = pltpu.get_barrier_semaphore()
    for dev in (partner, left, right):
        pl.semaphore_signal(barrier, inc=1, device_id={"pool": dev}, device_id_type=MESH)
    for t in range(PAIRS):
        start_qkv(0, t)
    for p in range(STAGE):
        page_copy(0, p).start()
    s_loc[...] = jnp.zeros_like(s_loc)
    s_send[...] = jnp.zeros_like(s_send)
    n_s[...] = jnp.zeros_like(n_s)
    own_rows = pl.ds(pl.multiple_of(core * tokens, tokens), tokens)
    x[own_rows, :] = hid[0]
    pl.semaphore_wait(barrier, 3)
    x_copy = remote(hid.at[0], x.at[own_rows], x_sem, partner)
    x_copy.start()
    raw[...] = jnp.zeros_like(raw)
    x_copy.wait()
    norm_only(gain_row(gain_a, 0))

    def layer(l, carry):
        for t in range(2):
            qkv_pair(l, t)
        for n in range(2):
            q_right(n).start()
            q_left(n).start()
        for n in range(2):
            q_part(n).start()
        for t in range(2, 6):
            qkv_pair(l, t)

        @pl.when(l == 0)
        def _():
            turn_pages(0, 0, n_pages)
        attend_new()
        q_right(0).wait_recv()
        q_right(2).start()
        q_part(2).start()
        q_left(0).wait_recv()
        q_left(2).start()
        q_part(5).start()
        attend_pages(own_unit, core, p_loc, s_loc)
        q_right(1).wait_recv()
        q_part(3).start()
        q_left(1).wait_recv()
        q_part(4).start()
        for n in range(n_col):
            wo_copy(l, n).start()
        for t in range(PAIRS):
            for sub in range(2):
                gu_copy(l, t, sub).start()
        attend_pages(near_first, core, p_loc, s_loc)
        for n in range(2, 6):
            q_part(n).wait_recv()
        attend_pages(near_first, other, p_send, s_send)
        start(o_part(LEFT, 0))
        start(o_part(RIGHT, 1))
        q_right(2).wait_recv()
        q_part(6).start()
        q_left(2).wait_recv()
        q_part(7).start()
        attend_pages(far_unit, core, p_loc, s_loc)
        merge_pair(LEFT, 0)
        start(o_left(0))
        merge_pair(RIGHT, 1)
        start(o_right(0))
        q_part(6).wait_recv()
        q_part(7).wait_recv()
        attend_pages(far_unit, other, p_send, s_send)
        start(o_part(FAR, 0))
        start(o_part(FAR, 1))
        for n in range(dim // COL):
            wd_copy(l, n).start()
        attend_pages(near_last, core, p_loc, s_loc)
        merge_pair(FAR, 0)
        start(o_right(1))
        merge_pair(FAR, 1)
        start(o_left(1))
        attend_pages(near_last, other, p_send, s_send)
        start(o_part(LEFT, 1))
        start(o_part(RIGHT, 0))
        q_part(0).wait_recv()
        q_part(1).wait_recv()
        attend_pages(own_unit, other, p_send, s_send)
        start(o_part(OWN, 0))
        start(o_part(OWN, 1))
        merge_pair(RIGHT, 0)
        merge_pair(LEFT, 1)
        for n in range(8):
            q_part(n).wait_send()
        for n in range(3):
            q_right(n).wait_send()
            q_left(n).wait_send()
        for j in range(CORES):
            merge_pair(OWN, j)
            merge(p_loc.at[OWN, j], s_loc.at[OWN, j], n_o.at[j], n_s.at[j])

        @pl.when(l + 1 < layers)
        def _():
            turn_pages(l + 1, 0, n_pages // 2)
        relay(o_right(1), 0, RIGHT, 0, o_right(2))
        relay(o_left(1), 1, LEFT, 1, o_left(2))
        wait_recv(o_right(0))
        merge(p_loc.at[OWN, 1], s_loc.at[OWN, 1], fin_o.at[0, 1], fin_s.at[0, 1])
        wait_recv(o_left(0))
        merge(p_loc.at[OWN, 0], s_loc.at[OWN, 0], fin_o.at[1, 0], fin_s.at[1, 0])

        @pl.when(l + 1 < layers)
        def _():
            turn_pages(l + 1, n_pages // 2, n_pages)
        finish(o_right(2), 0, 0)
        finish(o_left(2), 1, 1)
        for n in range(3):
            wait_send(o_right(n))
            wait_send(o_left(n))
        for d in range(4):
            for j in range(CORES):
                wait_send(o_part(d, j))

        def out_body(n, carry):
            wo_copy(l, n).wait()
            put_partial(n, 0, dot(att[...], wo_buf[n]))
            px_copy(0, n).start()
            return carry
        lax.fori_loop(0, dim // OUT_COL, out_body, 0)
        add_norm(0, gain_row(gain_m, l))

        def gate_block(j):
            gate, upper = raw[0], raw[1]
            val = gate / (1.0 + jnp.exp(-gate)) * upper
            col = lax.broadcasted_iota(jnp.int32, (rows, COL), 1) + j * COL
            val = jnp.where(col >= core * overlap, val, 0.0)
            inner[:, pl.ds(pl.multiple_of(j * COL, COL), COL)] = val.astype(BF)

        def gu_body(j, carry):
            for sub in range(2):
                gu_copy(l, j, sub).wait()
            sp = lax.rem(j, PAIRS)
            hv = h[...]
            gate = dot(hv, ring[2 * sp])
            upper = dot(hv, ring[2 * sp + 1])
            gate_block(jnp.maximum(j - 1, 0))
            raw[0] = gate
            raw[1] = upper

            @pl.when(j + PAIRS < ff_chunks)
            def _():
                for sub in range(2):
                    gu_copy(l, j + PAIRS, sub).start()

            @pl.when((j + PAIRS >= ff_chunks) & (l + 1 < layers))
            def _():
                start_qkv(l + 1, sp)
            return carry
        lax.fori_loop(0, ff_chunks, gu_body, 0)
        gate_block(ff_chunks - 1)

        def down_body(n, carry):
            iv = inner[...]
            for sub in range(OUT_COL // COL):
                wd_copy(l, 2 * n + sub).wait()
            for sub in range(OUT_COL // COL):
                put_partial(n, sub * (COL // hd), dot(iv, wd_buf[2 * n + sub]))
            px_copy(1, n).start()
            return carry
        lax.fori_loop(0, dim // OUT_COL, down_body, 0)
        add_norm(1, gain_row(gain_a, lax.rem(l + 1, layers)))
        return carry
    lax.fori_loop(0, layers, layer, 0)
    out[0] = x[own_rows, :]


def solution(mesh):
    group = mesh.shape["pool"]

    def local_program(kv, idx, hid, attn_norm, w_query, w_key, w_value, w_out, mlp_norm, w_gate, w_up, w_down):
        layers, n_pages, _, page_len, heads, hd = kv.shape
        slots = idx.shape[2]
        _, tokens, dim = hid.shape
        ff = w_gate.shape[2]
        half, rows = heads // CORES, CORES * tokens
        ff_cols = -(-ff // (CORES * COL)) * COL
        cosine, sine = rope_tables(group * slots * page_len, tokens, hd)
        cos2 = jnp.asarray(np.tile(cosine, (CORES, 1)))
        sin2 = jnp.asarray(np.tile(sine, (CORES, 1)))
        cfg = (layers, tokens, dim, heads, hd, ff, n_pages, slots)
        vmem = pl.BlockSpec(memory_space=pltpu.VMEM)
        hbm = pl.BlockSpec(memory_space=pl.ANY)
        smem = pl.BlockSpec(memory_space=pltpu.SMEM)
        dma = pltpu.SemaphoreType.DMA
        o_block = (half, tokens, hd)
        s_block = (tokens, 128)
        n_out = dim // OUT_COL
        scratch = [
            pltpu.VMEM((rows, dim), BF), pltpu.VMEM((rows, dim), BF), pltpu.VMEM((rows, half * hd), BF), pltpu.VMEM((rows, ff_cols), BF),
            pltpu.VMEM((CHIPS, CORES, 2, half // 2, CORES, tokens, hd), BF),
            pltpu.VMEM((half, CORES, tokens, hd), BF), pltpu.VMEM((half, CORES, tokens, hd), BF),
            pltpu.VMEM((n_pages, 2, heads, page_len, hd), BF),
            pltpu.VMEM((STAGE, 2, page_len, heads, hd), BF),
            pltpu.VMEM((2, heads * PITCH, hd), F32),
            pltpu.VMEM((4, CORES) + o_block, F32), pltpu.VMEM((4, CORES) + o_block, F32), pltpu.VMEM((4, CORES) + o_block, F32),
            pltpu.VMEM((4, CORES) + s_block, F32), pltpu.VMEM((4, CORES) + s_block, F32), pltpu.VMEM((4, CORES) + s_block, F32),
            pltpu.VMEM((CORES,) + o_block, F32), pltpu.VMEM((CORES,) + s_block, F32),
            pltpu.VMEM((2,) + o_block, F32), pltpu.VMEM((2,) + s_block, F32),
            pltpu.VMEM((2, CORES) + o_block, F32), pltpu.VMEM((2, CORES) + s_block, F32),
            pltpu.VMEM((2, n_out, CORES, OUT_COL // hd, tokens, hd), F32), pltpu.VMEM((2, rows, COL), F32),
            pltpu.VMEM((2 * PAIRS, dim, COL), BF), pltpu.VMEM((n_out, half * hd, OUT_COL), BF), pltpu.VMEM((dim // COL, ff_cols, COL), BF),
            dma((2 * PAIRS,)), dma((n_out,)), dma((dim // COL,)), dma((STAGE,)),
            dma((2,)), dma((8, 2)), dma((3, 2)), dma((3, 2)), dma((4, CORES, 2, 2)), dma((3, 3, 2)), dma((3, 3, 2)), dma((2, n_out, 2)),
        ]
        result = pl.pallas_call(
            functools.partial(kernel, cfg),
            out_shape=jax.ShapeDtypeStruct((1, tokens, dim), BF),
            in_specs=[smem] + [vmem] * 5 + [hbm] * 8,
            out_specs=vmem,
            scratch_shapes=scratch,
            compiler_params=pltpu.CompilerParams(collective_id=0, has_side_effects=True, vmem_limit_bytes=67043328),
            name="decoder",
        )(idx, hid, cos2, sin2, attn_norm, mlp_norm,
          kv, w_query, w_key, w_value, w_out, w_gate, w_up, w_down)
        return result

    data_specs = (P(None, ("rep", "pool")), P(None, ("rep", "pool"), None), P(("rep", "pool")))
    return jax.shard_map(local_program, mesh=mesh, in_specs=data_specs + (P(),) * 9, out_specs=P(("rep", "pool")), check_vma=False)
```

```python
import functools
import math
import numpy as np
import jax
import jax.numpy as jnp
from jax import lax
from jax.experimental import pallas as pl
from jax.experimental.pallas import tpu as pltpu
from jax.sharding import PartitionSpec as P

NORM_EPS = 1e-6
ROPE_BASE = 10000.0
LOG2E = 1.4426950408889634
NEG = -1e30
MESH = pl.DeviceIdType.MESH
BF = jnp.bfloat16
F32 = jnp.float32

CORES = 2
CHIPS = 4
COL = 256
PAIRS = 6
TURN = 2
PITCH = 36
OUT_COL = 512
GATE_WAIT = 1


def rope_tables(offset, tokens, head_dim):
    positions = (offset + np.arange(tokens)).astype(np.float32)
    exponent = np.arange(head_dim // 2).astype(np.float32) * np.float32(-2.0 / head_dim)
    inv_freq = np.power(np.float32(ROPE_BASE), exponent).astype(np.float32)
    angles = (positions[:, None] * inv_freq[None, :]).astype(np.float32)
    cosine, sine = np.cos(angles), np.sin(angles)
    return np.concatenate([cosine, cosine], 1), np.concatenate([-sine, sine], 1)


def kernel(cfg, idx, hid, cos, sin, gain_a, gain_m, kv, wq, wk, wv, wo, wg, wu, wd, out,
           x, h, att, inner, q, k_new, v_new, pages, unpack,
           p_loc, p_send, p_recv, s_loc, s_send, s_recv, t_loc, n_o, n_s,
           f_o, f_s, fin_o, fin_s, px_recv, raw, ring, wo_buf, wd_buf,
           ring_sem, wo_sem, wd_sem, page_sem,
           x_sem, qp_sem, qr_sem, ql_sem, po_sem, ro_sem, lo_sem, px_sem):
    layers, tokens, dim, heads, hd, ff, n_pages, slots = cfg
    group = CORES * CHIPS
    half = heads // CORES
    part = half // 2
    rows = CORES * tokens
    width = half * hd
    ff_cols = wd_buf.shape[1]
    ff_chunks = ff_cols // COL
    overlap = CORES * ff_cols - ff
    me = lax.axis_index("pool")
    chip = lax.div(me, CORES)
    core = lax.rem(me, CORES)
    partner = me + 1 - 2 * core
    right = lax.rem(me + CORES, group)
    left = lax.rem(me + group - CORES, group)
    c_right = lax.rem(chip + 1, CHIPS)
    c_left = lax.rem(chip + CHIPS - 1, CHIPS)
    c_far = lax.rem(chip + 2, CHIPS)
    other = 1 - core
    OWN, RIGHT, LEFT, FAR = 0, 1, 2, 3
    chip_of = {OWN: chip, RIGHT: c_right, LEFT: c_left, FAR: c_far}
    score_scale = LOG2E / math.sqrt(hd)

    def remote(src, dst, sem, dev):
        return pltpu.make_async_remote_copy(src_ref=src, dst_ref=dst, send_sem=sem.at[0], recv_sem=sem.at[1],
                                            device_id={"pool": dev}, device_id_type=MESH)

    def qkv_copy(l, t, w, sub):
        base = lax.rem(t, 2) * 2 * COL + sub * COL
        col = pl.multiple_of(core * width + base, COL)
        slot = 2 * t + sub
        return pltpu.make_async_copy(w.at[l, :, pl.ds(col, COL)], ring.at[slot], ring_sem.at[slot])

    def start_qkv(l, t):
        for n, w in enumerate((wq, wk, wv)):
            @pl.when(lax.div(t, 2) == n)
            def _(w=w):
                for sub in range(2):
                    qkv_copy(l, t, w, sub).start()

    def gu_copy(l, j, sub):
        col = pl.multiple_of(core * (ff - ff_cols) + j * COL, 128)
        slot = 2 * lax.rem(j, PAIRS) + sub
        return pltpu.make_async_copy((wg, wu)[sub].at[l, :, pl.ds(col, COL)], ring.at[slot], ring_sem.at[slot])

    def wo_copy(l, n):
        return pltpu.make_async_copy(wo.at[l, pl.ds(pl.multiple_of(core * width, width), width), pl.ds(pl.multiple_of(n * OUT_COL, OUT_COL), OUT_COL)],
                                     wo_buf.at[n], wo_sem.at[n])

    def wd_copy(l, n):
        row = pl.multiple_of(core * (ff - ff_cols), 128)
        return pltpu.make_async_copy(wd.at[l, pl.ds(row, ff_cols), pl.ds(pl.multiple_of(n * COL, COL), COL)],
                                     wd_buf.at[n], wd_sem.at[n])

    page_len = kv.shape[3] // heads

    def page_copy(l, p):
        return pltpu.make_async_copy(kv.at[l, p], pages.at[p], page_sem.at[p])

    def start_pages(l):
        def body(p, carry):
            page_copy(l, p).start()
            return carry
        lax.fori_loop(0, n_pages, body, 0)

    def turn_pages(l, lo, hi):
        def body(t, carry):
            for e in range(TURN):
                page_copy(l, TURN * t + e).wait()
            for e in range(TURN):
                for b in range(2):
                    for r in range(page_len):
                        unpack[e, b, pl.ds(r, heads, stride=PITCH), :] = pages[TURN * t + e, b, r * heads:(r + 1) * heads].astype(F32)
            for e in range(TURN):
                for b in range(2):
                    for i in range(heads):
                        pages[TURN * t + e, b, i * page_len:(i + 1) * page_len] = unpack[e, b, pl.ds(i * PITCH, page_len), :].astype(BF)
            return carry
        lax.fori_loop(lo // TURN, hi // TURN, body, 0)

    def q_right(n):
        src = (q.at[chip, core, 0], q.at[chip, core, 1], q.at[c_left, core, 0])[n]
        return remote(src, src, qr_sem.at[n], right)

    def q_left(n):
        src = (q.at[chip, core, 1], q.at[chip, core, 0], q.at[c_right, core, 1])[n]
        return remote(src, src, ql_sem.at[n], left)

    def q_part(n):
        src = (q.at[chip, core, 0], q.at[chip, core, 1], q.at[c_left, core, 0], q.at[c_left, core, 1],
               q.at[c_right, core, 0], q.at[c_right, core, 1], q.at[c_far, core, 0], q.at[c_far, core, 1])[n]
        return remote(src, src, qp_sem.at[n], partner)

    def o_part(d, j):
        return (remote(p_send.at[d, j], p_recv.at[d, j], po_sem.at[d, j, 0], partner),
                remote(s_send.at[d, j], s_recv.at[d, j], po_sem.at[d, j, 1], partner))

    def message(d, j, dst_o, dst_s, sem, dev):
        lo, hi = pl.ds(0, part), pl.ds(part, part)
        return (remote(t_loc.at[d, j], dst_s, sem.at[0], dev), remote(p_loc.at[d, j, lo], dst_o.at[lo], sem.at[1], dev),
                remote(p_loc.at[d, j, hi], dst_o.at[hi], sem.at[2], dev))

    def o_right(n):
        d, j, dst_o, dst_s = ((RIGHT, 1, fin_o.at[0, 1], fin_s.at[0, 1]), (FAR, 0, f_o.at[0], f_s.at[0]),
                              (RIGHT, 0, fin_o.at[0, 0], fin_s.at[0, 0]))[n]
        return message(d, j, dst_o, dst_s, ro_sem.at[n], right)

    def o_left(n):
        d, j, dst_o, dst_s = ((LEFT, 0, fin_o.at[1, 0], fin_s.at[1, 0]), (FAR, 1, f_o.at[1], f_s.at[1]),
                              (LEFT, 1, fin_o.at[1, 1], fin_s.at[1, 1]))[n]
        return message(d, j, dst_o, dst_s, lo_sem.at[n], left)

    def px_copy(which, n):
        return remote(p_send.at[n, :, pl.ds(0, OUT_COL // hd)], px_recv.at[which, n], px_sem.at[which, n], partner)

    def put_partial(n, first, v):
        for j in range(CORES):
            for c in range(v.shape[1] // hd):
                p_send[n, j, first + c] = v[j * tokens:(j + 1) * tokens, c * hd:(c + 1) * hd]

    def start(copies):
        for cp in copies:
            cp.start()

    def wait_recv(copies):
        for cp in copies:
            cp.wait_recv()

    def wait_send(copies):
        for cp in copies:
            cp.wait_send()

    lane = lax.broadcasted_iota(jnp.int32, (tokens, 128), 1)

    def attention(blocks, stats, mask=None):
        scores = [lax.dot_general(qv, kk(), (((1,), (1,)), ((), ())), preferred_element_type=F32) for _, qv, kk, _, _ in blocks]
        scores = [s * score_scale for s in scores]
        if mask is not None:
            scores = [jnp.where(mask, s, NEG) for s in scores]
        tops = [jnp.max(s, axis=1, keepdims=True) for s in scores]
        probs = [jnp.exp2(s - m) for s, m in zip(scores, tops)]
        sums = [jnp.sum(p, axis=1, keepdims=True) for p in probs]
        probs = [p.astype(BF) for p in probs]
        for (i, _, _, vv, store), p in zip(blocks, probs):
            store(jnp.dot(p, vv(), preferred_element_type=F32))
        for (i, _, _, _, _), m, z in zip(blocks, tops, sums):
            stats = jnp.where(lane == i, m, jnp.where(lane == half + i, z, stats))
        return stats

    def attend_pages(unit, hb, o_ref, s_ref):
        def body(t, carry):
            d, ca, j = unit(t)
            where = [idx[CORES * ca + j, 0, s] for s in range(slots)]
            blocks = []
            for i in range(half):
                def load(b, head=hb * half + i):
                    return jnp.concatenate([pages[w, b, pl.ds(pl.multiple_of(head * page_len, page_len), page_len)] for w in where], axis=0)

                def store(o, i=i):
                    o_ref[d, j, i] = o
                blocks.append((i, q[ca, hb, j, i], functools.partial(load, 0), functools.partial(load, 1), store))
            s_ref[d, j] = attention(blocks, s_ref[d, j])
            return carry
        lax.fori_loop(0, CORES, body, 0)

    def own_unit(t):
        return OWN, chip, t

    def far_unit(t):
        return FAR, c_far, t

    def near_first(t):
        return LEFT - t, lax.rem(chip + CHIPS - 1 + 2 * t, CHIPS), t

    def near_last(t):
        return LEFT - t, lax.rem(chip + CHIPS - 1 + 2 * t, CHIPS), 1 - t

    def attend_new():
        row = lax.broadcasted_iota(jnp.int32, (tokens, tokens), 0)
        col = lax.broadcasted_iota(jnp.int32, (tokens, tokens), 1)
        mask = col <= row

        def body(j, carry):
            blocks = []
            for i in range(half):
                def store(o, i=i):
                    n_o[j, i] = o
                blocks.append((i, q[chip, core, j, i], lambda i=i: k_new[i, j], lambda i=i: v_new[i, j], store))
            n_s[j] = attention(blocks, n_s[j], mask)
            return carry
        lax.fori_loop(0, CORES, body, 0)

    def weights(sa, sb):
        m = jnp.maximum(sa, sb)
        wa, wb = jnp.exp2(sa - m), jnp.exp2(sb - m)
        z = sa * pltpu.roll(wa, half, axis=1) + sb * pltpu.roll(wb, half, axis=1)
        return wa, wb, jnp.where(lane < half, m, jnp.where(lane < 2 * half, z, 0.0))

    def blend(ao, bo, wa, wb, i):
        return ao[i] * wa[:, i:i + 1] + bo[i] * wb[:, i:i + 1]

    def merge(ao, a_s, bo, sb):
        wa, wb, a_s[...] = weights(a_s[...], sb)
        for i in range(half):
            ao[i] = blend(ao, bo, wa, wb, i)

    def pack(v):
        out_v = v[0:8]
        for r in range(1, tokens // 8):
            out_v = out_v + pltpu.roll(v[8 * r:8 * r + 8], 2 * half * r, axis=1)
        return out_v

    def unpacked(v):
        blocks = [v] + [pltpu.roll(v, 128 - 2 * half * r, axis=1) for r in range(1, tokens // 8)]
        return jnp.where(lane < 2 * half, jnp.concatenate(blocks, axis=0), 0.0)

    def send(d, j, copies):
        t_loc[d, j] = pack(s_loc[d, j])
        start(copies)

    def merge_pair(d, j):
        wait_recv(o_part(d, j))
        merge(p_loc.at[d, j], s_loc.at[d, j], p_recv.at[d, j], s_recv[d, j])

    def relay_first(copies, side, d, j, onward):
        wait_recv(copies[:2])
        wa, wb, s_loc[d, j] = weights(s_loc[d, j], unpacked(f_s[side]))
        for i in range(part):
            p_loc[d, j, i] = blend(p_loc.at[d, j], f_o.at[side], wa, wb, i)
        send(d, j, onward[:2])
        return wa, wb

    def relay_last(copies, side, d, j, onward, scales):
        wait_recv(copies[2:])
        for i in range(part, half):
            p_loc[d, j, i] = blend(p_loc.at[d, j], f_o.at[side], *scales, i)
        start(onward[2:])

    def finish(ready, side, j, lo, hi, scales=None):
        wait_recv(ready)
        if scales is None:
            wa, wb, st = weights(s_loc[OWN, j], unpacked(fin_s[side, j]))
            scales = (wa, wb, 1.0 / st)
        wa, wb, inv = scales
        for i in range(lo, hi):
            o = blend(p_loc.at[OWN, j], fin_o.at[side, j], wa, wb, i) * inv[:, half + i:half + i + 1]
            att[j * tokens:(j + 1) * tokens, i * hd:(i + 1) * hd] = o.astype(BF)
        return scales

    ROWS = 16
    n_col = dim // OUT_COL

    def normalise(squares, gain):
        inv = lax.rsqrt(jnp.sum(squares, axis=1, keepdims=True) * (1.0 / dim) + NORM_EPS)
        for r in range(0, rows, ROWS):
            h[r:r + ROWS, :] = (x[r:r + ROWS, :].astype(F32) * inv[r:r + ROWS] * gain).astype(BF)

    def square_tiles(v):
        v = v * v
        return sum(v[:, c:c + 128] for c in range(0, v.shape[1], 128))

    def gain_row(ref, l):
        g = ref[0:1, :].astype(F32)
        for n in range(1, layers):
            g = jnp.where(l == n, ref[n:n + 1, :].astype(F32), g)
        return g

    def norm_only(gain):
        normalise(square_tiles(x[...].astype(F32)), gain)

    def add_norm(which, gain):
        squares = jnp.zeros((rows, 128), F32)
        for n in range(n_col):
            px_copy(which, n).wait()
            for c in range(OUT_COL // hd):
                cols = slice(n * OUT_COL + c * hd, n * OUT_COL + (c + 1) * hd)
                total = jnp.concatenate([p_send[n, j, c] + px_recv[which, n, j, c] for j in range(CORES)], axis=0)
                xv = (x[:, cols].astype(F32) + total).astype(BF)
                x[:, cols] = xv
                xv = xv.astype(F32)
                squares = squares + xv * xv
        normalise(squares, gain)

    def dot(a, b):
        return jnp.dot(a, b, preferred_element_type=F32)

    def wait_qkv(l, lo, hi):
        for t in range(lo, hi):
            for sub in range(2):
                qkv_copy(l, t, (wq, wk, wv)[t // 2], sub).wait()

    def qkv_pair(l, t):
        hv = h[...]
        for sub in range(2):
            res = dot(hv, ring[2 * t + sub])
            for e in range(COL // hd):
                v = res[:, e * hd:(e + 1) * hd]
                if t < 4:
                    v = v * cos[...] + pltpu.roll(v, hd // 2, axis=1) * sin[...]
                v = v.astype(BF)
                i = (t % 2) * part + sub * (COL // hd) + e
                for j in range(CORES):
                    vj = v[j * tokens:(j + 1) * tokens]
                    if t < 2:
                        q[chip, core, j, i] = vj
                    elif t < 4:
                        k_new[i, j] = vj
                    else:
                        v_new[i, j] = vj
    barrier = pltpu.get_barrier_semaphore()
    for dev in (partner, left, right):
        pl.semaphore_signal(barrier, inc=1, device_id={"pool": dev}, device_id_type=MESH)
    for t in range(PAIRS):
        start_qkv(0, t)
    start_pages(0)
    s_loc[...] = jnp.zeros_like(s_loc)
    s_send[...] = jnp.zeros_like(s_send)
    n_s[...] = jnp.zeros_like(n_s)
    own_rows = pl.ds(pl.multiple_of(core * tokens, tokens), tokens)
    x[own_rows, :] = hid[0]
    pl.semaphore_wait(barrier, 3)
    x_copy = remote(hid.at[0], x.at[own_rows], x_sem, partner)
    x_copy.start()
    raw[...] = jnp.zeros_like(raw)
    x_copy.wait()
    norm_only(gain_row(gain_a, 0))

    def layer(l, carry):
        wait_qkv(l, 0, 2)
        for t in range(2):
            qkv_pair(l, t)
        for n in range(2):
            q_right(n).start()
            q_left(n).start()
        for n in range(2):
            q_part(n).start()
        wait_qkv(l, 2, 6)
        for t in range(2, 6):
            qkv_pair(l, t)

        @pl.when(l == 0)
        def _():
            turn_pages(0, 0, n_pages)
        attend_pages(own_unit, core, p_loc, s_loc)
        attend_new()
        q_right(0).wait_recv()
        q_right(2).start()
        q_part(2).start()
        q_left(0).wait_recv()
        q_left(2).start()
        q_part(5).start()
        attend_pages(near_first, core, p_loc, s_loc)
        q_part(2).wait_recv()
        q_part(5).wait_recv()
        attend_pages(near_first, other, p_send, s_send)
        start(o_part(LEFT, 0))
        start(o_part(RIGHT, 1))
        q_right(1).wait_recv()
        q_part(3).start()
        q_left(1).wait_recv()
        q_part(4).start()
        attend_pages(near_last, core, p_loc, s_loc)
        merge_pair(LEFT, 0)
        send(LEFT, 0, o_left(0))
        merge_pair(RIGHT, 1)
        send(RIGHT, 1, o_right(0))
        q_part(3).wait_recv()
        q_part(4).wait_recv()
        for n in range(n_col):
            wo_copy(l, n).start()
        for t in range(PAIRS):
            for sub in range(2):
                gu_copy(l, t, sub).start()
        attend_pages(near_last, other, p_send, s_send)
        start(o_part(LEFT, 1))
        start(o_part(RIGHT, 0))
        q_right(2).wait_recv()
        q_part(6).start()
        q_left(2).wait_recv()
        q_part(7).start()
        attend_pages(far_unit, core, p_loc, s_loc)
        q_part(6).wait_recv()
        q_part(7).wait_recv()
        attend_pages(far_unit, other, p_send, s_send)
        start(o_part(FAR, 0))
        start(o_part(FAR, 1))
        q_part(0).wait_recv()
        q_part(1).wait_recv()
        attend_pages(own_unit, other, p_send, s_send)
        start(o_part(OWN, 0))
        start(o_part(OWN, 1))
        merge_pair(FAR, 0)
        send(FAR, 0, o_right(1))
        merge_pair(FAR, 1)
        send(FAR, 1, o_left(1))

        @pl.when(l + 1 < layers)
        def _():
            start_pages(l + 1)
        merge_pair(RIGHT, 0)
        merge_pair(LEFT, 1)
        for n in range(8):
            q_part(n).wait_send()
        for n in range(3):
            q_right(n).wait_send()
            q_left(n).wait_send()
        for j in range(CORES):
            merge_pair(OWN, j)
            merge(p_loc.at[OWN, j], s_loc.at[OWN, j], n_o.at[j], n_s[j])

        @pl.when(l + 1 < layers)
        def _():
            turn_pages(l + 1, 0, n_pages // 2)
        from_left = relay_first(o_right(1), 0, RIGHT, 0, o_right(2))
        from_right = relay_first(o_left(1), 1, LEFT, 1, o_left(2))
        relay_last(o_right(1), 0, RIGHT, 0, o_right(2), from_left)
        relay_last(o_left(1), 1, LEFT, 1, o_left(2), from_right)
        for n in range(dim // COL):
            wd_copy(l, n).start()
        wait_recv(o_right(0))
        merge(p_loc.at[OWN, 1], s_loc.at[OWN, 1], fin_o.at[0, 1], unpacked(fin_s[0, 1]))
        wait_recv(o_left(0))
        merge(p_loc.at[OWN, 0], s_loc.at[OWN, 0], fin_o.at[1, 0], unpacked(fin_s[1, 0]))

        @pl.when(l + 1 < layers)
        def _():
            turn_pages(l + 1, n_pages // 2, n_pages)
        first = finish(o_right(2)[:2], 0, 0, 0, part)
        second = finish(o_left(2)[:2], 1, 1, 0, part)
        finish(o_right(2)[2:], 0, 0, part, half, first)
        finish(o_left(2)[2:], 1, 1, part, half, second)
        for n in range(3):
            wait_send(o_right(n))
            wait_send(o_left(n))
        for d in range(4):
            for j in range(CORES):
                wait_send(o_part(d, j))

        for n in range(n_col):
            wo_copy(l, n).wait()
        for n in range(n_col):
            put_partial(n, 0, dot(att[...], wo_buf[n]))
            px_copy(0, n).start()
        add_norm(0, gain_row(gain_m, l))

        def gate_block(j):
            gate, upper = raw[0], raw[1]
            val = gate / (1.0 + jnp.exp(-gate)) * upper
            if j * COL < overlap:
                col = lax.broadcasted_iota(jnp.int32, (rows, COL), 1) + j * COL
                val = jnp.where(col >= core * overlap, val, 0.0)
            inner[:, j * COL:(j + 1) * COL] = val.astype(BF)

        for j in range(ff_chunks):
            if j % GATE_WAIT == 0:
                for jj in range(j, min(j + GATE_WAIT, ff_chunks)):
                    for sub in range(2):
                        gu_copy(l, jj, sub).wait()
            sp = j % PAIRS
            hv = h[...]
            gate = dot(hv, ring[2 * sp])
            upper = dot(hv, ring[2 * sp + 1])
            if j > 0:
                gate_block(j - 1)
            raw[0] = gate
            raw[1] = upper
            if j + PAIRS < ff_chunks:
                for sub in range(2):
                    gu_copy(l, j + PAIRS, sub).start()
            else:
                @pl.when(l + 1 < layers)
                def _(sp=sp):
                    for sub in range(2):
                        qkv_copy(l + 1, sp, (wq, wk, wv)[sp // 2], sub).start()
        gate_block(ff_chunks - 1)

        for n in range(dim // COL):
            wd_copy(l, n).wait()
        iv = inner[...]
        for n in range(n_col):
            for sub in range(OUT_COL // COL):
                put_partial(n, sub * (COL // hd), dot(iv, wd_buf[2 * n + sub]))
            px_copy(1, n).start()
        add_norm(1, gain_row(gain_a, lax.rem(l + 1, layers)))
        return carry
    lax.fori_loop(0, layers, layer, 0)
    out[0] = x[own_rows, :]


def solution(mesh):
    group = mesh.shape["pool"]

    def local_program(kv, idx, hid, attn_norm, w_query, w_key, w_value, w_out, mlp_norm, w_gate, w_up, w_down):
        layers, n_pages, _, page_len, heads, hd = kv.shape
        slots = idx.shape[2]
        _, tokens, dim = hid.shape
        ff = w_gate.shape[2]
        half, rows = heads // CORES, CORES * tokens
        ff_cols = -(-ff // (CORES * COL)) * COL
        cosine, sine = rope_tables(group * slots * page_len, tokens, hd)
        cos2 = jnp.asarray(np.tile(cosine, (CORES, 1)))
        sin2 = jnp.asarray(np.tile(sine, (CORES, 1)))
        cfg = (layers, tokens, dim, heads, hd, ff, n_pages, slots)
        vmem = pl.BlockSpec(memory_space=pltpu.VMEM)
        hbm = pl.BlockSpec(memory_space=pl.ANY)
        smem = pl.BlockSpec(memory_space=pltpu.SMEM)
        dma = pltpu.SemaphoreType.DMA
        o_block = (half, tokens, hd)
        s_block, t_block = (tokens, 128), (8, 128)
        n_out = dim // OUT_COL
        scratch = [
            pltpu.VMEM((rows, dim), BF), pltpu.VMEM((rows, dim), BF), pltpu.VMEM((rows, half * hd), BF), pltpu.VMEM((rows, ff_cols), BF),
            pltpu.VMEM((CHIPS, CORES, CORES, half, tokens, hd), BF),
            pltpu.VMEM((half, CORES, tokens, hd), BF), pltpu.VMEM((half, CORES, tokens, hd), BF),
            pltpu.VMEM((n_pages, 2, page_len * heads, hd), BF),
            pltpu.VMEM((TURN, 2, heads * PITCH, hd), F32),
            pltpu.VMEM((4, CORES) + o_block, F32), pltpu.VMEM((4, CORES) + o_block, F32), pltpu.VMEM((4, CORES) + o_block, F32),
            pltpu.VMEM((4, CORES) + s_block, F32), pltpu.VMEM((4, CORES) + s_block, F32), pltpu.VMEM((4, CORES) + s_block, F32),
            pltpu.VMEM((4, CORES) + t_block, F32),
            pltpu.VMEM((CORES,) + o_block, F32), pltpu.VMEM((CORES,) + s_block, F32),
            pltpu.VMEM((2,) + o_block, F32), pltpu.VMEM((2,) + t_block, F32),
            pltpu.VMEM((2, CORES) + o_block, F32), pltpu.VMEM((2, CORES) + t_block, F32),
            pltpu.VMEM((2, n_out, CORES, OUT_COL // hd, tokens, hd), F32), pltpu.VMEM((2, rows, COL), F32),
            pltpu.VMEM((2 * PAIRS, dim, COL), BF), pltpu.VMEM((n_out, half * hd, OUT_COL), BF), pltpu.VMEM((dim // COL, ff_cols, COL), BF),
            dma((2 * PAIRS,)), dma((n_out,)), dma((dim // COL,)), dma((n_pages,)),
            dma((2,)), dma((8, 2)), dma((3, 2)), dma((3, 2)), dma((4, CORES, 2, 2)), dma((3, 3, 2)), dma((3, 3, 2)), dma((2, n_out, 2)),
        ]
        result = pl.pallas_call(
            functools.partial(kernel, cfg),
            out_shape=jax.ShapeDtypeStruct((1, tokens, dim), BF),
            in_specs=[smem] + [vmem] * 5 + [hbm] * 8,
            out_specs=vmem,
            scratch_shapes=scratch,
            compiler_params=pltpu.CompilerParams(collective_id=0, has_side_effects=True, vmem_limit_bytes=67043328),
            name="decoder",
        )(idx, hid, cos2, sin2, attn_norm, mlp_norm,
          kv.reshape(layers, n_pages, 2, page_len * heads, hd), w_query, w_key, w_value, w_out, w_gate, w_up, w_down)
        return result

    data_specs = (P(None, ("rep", "pool")), P(None, ("rep", "pool"), None), P(("rep", "pool")))
    return jax.shard_map(local_program, mesh=mesh, in_specs=data_specs + (P(),) * 9, out_specs=P(("rep", "pool")), check_vma=False)
```

```python
import functools
import math
import numpy as np
import jax
import jax.numpy as jnp
from jax import lax
from jax.experimental import pallas as pl
from jax.experimental.pallas import tpu as pltpu
from jax.sharding import PartitionSpec as P

NORM_EPS = 1e-6
ROPE_BASE = 10000.0
LOG2E = 1.4426950408889634
NEG = -1e30
MESH = pl.DeviceIdType.MESH
BF = jnp.bfloat16
F32 = jnp.float32

CORES = 2
CHIPS = 4
COL = 256
PAIRS = 6
TURN = 2
PITCH = 36
OUT_COL = 512
GATE_WAIT = 1


def rope_tables(offset, tokens, head_dim):
    positions = (offset + np.arange(tokens)).astype(np.float32)
    exponent = np.arange(head_dim // 2).astype(np.float32) * np.float32(-2.0 / head_dim)
    inv_freq = np.power(np.float32(ROPE_BASE), exponent).astype(np.float32)
    angles = (positions[:, None] * inv_freq[None, :]).astype(np.float32)
    cosine, sine = np.cos(angles), np.sin(angles)
    return np.concatenate([cosine, cosine], 1), np.concatenate([-sine, sine], 1)


def kernel(cfg, idx, hid, cos, sin, gain_a, gain_m, kv, wq, wk, wv, wo, wg, wu, wd, out,
           x, h, att, inner, q, k_new, v_new, pages, unpack,
           p_loc, p_send, p_recv, s_loc, s_send, s_recv, t_loc, n_o, n_s,
           f_o, f_s, fin_o, fin_s, px_recv, raw, ring, wo_buf, wd_buf,
           ring_sem, wo_sem, wd_sem, page_sem,
           x_sem, qp_sem, qr_sem, ql_sem, po_sem, ro_sem, lo_sem, px_sem):
    layers, tokens, dim, heads, hd, ff, n_pages, slots = cfg
    group = CORES * CHIPS
    half = heads // CORES
    part = half // 2
    rows = CORES * tokens
    width = half * hd
    ff_cols = wd_buf.shape[1]
    ff_chunks = ff_cols // COL
    overlap = CORES * ff_cols - ff
    me = lax.axis_index("pool")
    chip = lax.div(me, CORES)
    core = lax.rem(me, CORES)
    partner = me + 1 - 2 * core
    right = lax.rem(me + CORES, group)
    left = lax.rem(me + group - CORES, group)
    c_right = lax.rem(chip + 1, CHIPS)
    c_left = lax.rem(chip + CHIPS - 1, CHIPS)
    c_far = lax.rem(chip + 2, CHIPS)
    other = 1 - core
    OWN, RIGHT, LEFT, FAR = 0, 1, 2, 3
    chip_of = {OWN: chip, RIGHT: c_right, LEFT: c_left, FAR: c_far}
    score_scale = LOG2E / math.sqrt(hd)

    def remote(src, dst, sem, dev):
        return pltpu.make_async_remote_copy(src_ref=src, dst_ref=dst, send_sem=sem.at[0], recv_sem=sem.at[1],
                                            device_id={"pool": dev}, device_id_type=MESH)

    def qkv_copy(l, t, w, sub):
        base = lax.rem(t, 2) * 2 * COL + sub * COL
        col = pl.multiple_of(core * width + base, COL)
        slot = 2 * t + sub
        return pltpu.make_async_copy(w.at[l, :, pl.ds(col, COL)], ring.at[slot], ring_sem.at[slot])

    def start_qkv(l, t):
        for n, w in enumerate((wq, wk, wv)):
            @pl.when(lax.div(t, 2) == n)
            def _(w=w):
                for sub in range(2):
                    qkv_copy(l, t, w, sub).start()

    def gu_copy(l, j, sub):
        col = pl.multiple_of(core * (ff - ff_cols) + j * COL, 128)
        slot = 2 * lax.rem(j, PAIRS) + sub
        return pltpu.make_async_copy((wg, wu)[sub].at[l, :, pl.ds(col, COL)], ring.at[slot], ring_sem.at[slot])

    def wo_copy(l, n):
        return pltpu.make_async_copy(wo.at[l, pl.ds(pl.multiple_of(core * width, width), width), pl.ds(pl.multiple_of(n * OUT_COL, OUT_COL), OUT_COL)],
                                     wo_buf.at[n], wo_sem.at[n])

    def wd_copy(l, n):
        row = pl.multiple_of(core * (ff - ff_cols), 128)
        return pltpu.make_async_copy(wd.at[l, pl.ds(row, ff_cols), pl.ds(pl.multiple_of(n * COL, COL), COL)],
                                     wd_buf.at[n], wd_sem.at[n])

    page_len = kv.shape[3] // heads

    def page_copy(l, p):
        return pltpu.make_async_copy(kv.at[l, p], pages.at[p], page_sem.at[p])

    def start_pages(l):
        def body(p, carry):
            page_copy(l, p).start()
            return carry
        lax.fori_loop(0, n_pages, body, 0)

    def turn_pages(l, lo, hi):
        def body(t, carry):
            for e in range(TURN):
                page_copy(l, TURN * t + e).wait()
            for e in range(TURN):
                for b in range(2):
                    for r in range(page_len):
                        unpack[e, b, pl.ds(r, heads, stride=PITCH), :] = pages[TURN * t + e, b, r * heads:(r + 1) * heads].astype(F32)
            for e in range(TURN):
                for b in range(2):
                    for i in range(heads):
                        pages[TURN * t + e, b, i * page_len:(i + 1) * page_len] = unpack[e, b, pl.ds(i * PITCH, page_len), :].astype(BF)
            return carry
        lax.fori_loop(lo // TURN, hi // TURN, body, 0)

    def q_right(n):
        src = (q.at[chip, core, 0], q.at[chip, core, 1], q.at[c_left, core, 0])[n]
        return remote(src, src, qr_sem.at[n], right)

    def q_left(n):
        src = (q.at[chip, core, 1], q.at[chip, core, 0], q.at[c_right, core, 1])[n]
        return remote(src, src, ql_sem.at[n], left)

    def q_part(n):
        src = (q.at[chip, core, 0], q.at[chip, core, 1], q.at[c_left, core, 0], q.at[c_left, core, 1],
               q.at[c_right, core, 0], q.at[c_right, core, 1], q.at[c_far, core, 0], q.at[c_far, core, 1])[n]
        return remote(src, src, qp_sem.at[n], partner)

    def o_part(d, j):
        return (remote(p_send.at[d, j], p_recv.at[d, j], po_sem.at[d, j, 0], partner),
                remote(s_send.at[d, j], s_recv.at[d, j], po_sem.at[d, j, 1], partner))

    def message(d, j, dst_o, dst_s, sem, dev):
        lo, hi = pl.ds(0, part), pl.ds(part, part)
        return (remote(t_loc.at[d, j], dst_s, sem.at[0], dev), remote(p_loc.at[d, j, lo], dst_o.at[lo], sem.at[1], dev),
                remote(p_loc.at[d, j, hi], dst_o.at[hi], sem.at[2], dev))

    def o_right(n):
        d, j, dst_o, dst_s = ((RIGHT, 1, fin_o.at[0, 1], fin_s.at[0, 1]), (FAR, 0, f_o.at[0], f_s.at[0]),
                              (RIGHT, 0, fin_o.at[0, 0], fin_s.at[0, 0]))[n]
        return message(d, j, dst_o, dst_s, ro_sem.at[n], right)

    def o_left(n):
        d, j, dst_o, dst_s = ((LEFT, 0, fin_o.at[1, 0], fin_s.at[1, 0]), (FAR, 1, f_o.at[1], f_s.at[1]),
                              (LEFT, 1, fin_o.at[1, 1], fin_s.at[1, 1]))[n]
        return message(d, j, dst_o, dst_s, lo_sem.at[n], left)

    def px_copy(which, n):
        return remote(p_send.at[n, :, pl.ds(0, OUT_COL // hd)], px_recv.at[which, n], px_sem.at[which, n], partner)

    def put_partial(n, first, v):
        for j in range(CORES):
            for c in range(v.shape[1] // hd):
                p_send[n, j, first + c] = v[j * tokens:(j + 1) * tokens, c * hd:(c + 1) * hd]

    def start(copies):
        for cp in copies:
            cp.start()

    def wait_recv(copies):
        for cp in copies:
            cp.wait_recv()

    def wait_send(copies):
        for cp in copies:
            cp.wait_send()

    lane = lax.broadcasted_iota(jnp.int32, (tokens, 128), 1)

    def attention(blocks, stats, mask=None):
        scores = [lax.dot_general(qv, kk(), (((1,), (1,)), ((), ())), preferred_element_type=F32) for _, qv, kk, _, _ in blocks]
        scores = [s * score_scale for s in scores]
        if mask is not None:
            scores = [jnp.where(mask, s, NEG) for s in scores]
        tops = [jnp.max(s, axis=1, keepdims=True) for s in scores]
        probs = [jnp.exp2(s - m) for s, m in zip(scores, tops)]
        sums = [jnp.sum(p, axis=1, keepdims=True) for p in probs]
        probs = [p.astype(BF) for p in probs]
        for (i, _, _, vv, store), p in zip(blocks, probs):
            store(jnp.dot(p, vv(), preferred_element_type=F32))
        for (i, _, _, _, _), m, z in zip(blocks, tops, sums):
            stats = jnp.where(lane == i, m, jnp.where(lane == half + i, z, stats))
        return stats

    def attend_pages(unit, hb, o_ref, s_ref):
        def body(t, carry):
            d, ca, j = unit(t)
            where = [idx[CORES * ca + j, 0, s] for s in range(slots)]
            blocks = []
            for i in range(half):
                def load(b, head=hb * half + i):
                    return jnp.concatenate([pages[w, b, pl.ds(pl.multiple_of(head * page_len, page_len), page_len)] for w in where], axis=0)

                def store(o, i=i):
                    o_ref[d, j, i] = o
                blocks.append((i, q[ca, hb, j, i], functools.partial(load, 0), functools.partial(load, 1), store))
            s_ref[d, j] = attention(blocks, s_ref[d, j])
            return carry
        lax.fori_loop(0, CORES, body, 0)

    def own_unit(t):
        return OWN, chip, t

    def far_unit(t):
        return FAR, c_far, t

    def near_first(t):
        return LEFT - t, lax.rem(chip + CHIPS - 1 + 2 * t, CHIPS), t

    def near_last(t):
        return LEFT - t, lax.rem(chip + CHIPS - 1 + 2 * t, CHIPS), 1 - t

    def attend_new():
        row = lax.broadcasted_iota(jnp.int32, (tokens, tokens), 0)
        col = lax.broadcasted_iota(jnp.int32, (tokens, tokens), 1)
        mask = col <= row

        def body(j, carry):
            blocks = []
            for i in range(half):
                def store(o, i=i):
                    n_o[j, i] = o
                blocks.append((i, q[chip, core, j, i], lambda i=i: k_new[i, j], lambda i=i: v_new[i, j], store))
            n_s[j] = attention(blocks, n_s[j], mask)
            return carry
        lax.fori_loop(0, CORES, body, 0)

    def weights(sa, sb):
        m = jnp.maximum(sa, sb)
        wa, wb = jnp.exp2(sa - m), jnp.exp2(sb - m)
        z = sa * pltpu.roll(wa, half, axis=1) + sb * pltpu.roll(wb, half, axis=1)
        return wa, wb, jnp.where(lane < half, m, jnp.where(lane < 2 * half, z, 0.0))

    def blend(ao, bo, wa, wb, i):
        return ao[i] * wa[:, i:i + 1] + bo[i] * wb[:, i:i + 1]

    def merge(ao, a_s, bo, sb):
        wa, wb, a_s[...] = weights(a_s[...], sb)
        for i in range(half):
            ao[i] = blend(ao, bo, wa, wb, i)

    def pack(v):
        out_v = v[0:8]
        for r in range(1, tokens // 8):
            out_v = out_v + pltpu.roll(v[8 * r:8 * r + 8], 2 * half * r, axis=1)
        return out_v

    def unpacked(v):
        blocks = [v] + [pltpu.roll(v, 128 - 2 * half * r, axis=1) for r in range(1, tokens // 8)]
        return jnp.where(lane < 2 * half, jnp.concatenate(blocks, axis=0), 0.0)

    def send(d, j, copies):
        t_loc[d, j] = pack(s_loc[d, j])
        start(copies)

    def merge_pair(d, j):
        wait_recv(o_part(d, j))
        merge(p_loc.at[d, j], s_loc.at[d, j], p_recv.at[d, j], s_recv[d, j])

    def relay_first(copies, side, d, j, onward):
        wait_recv(copies[:2])
        wa, wb, s_loc[d, j] = weights(s_loc[d, j], unpacked(f_s[side]))
        for i in range(part):
            p_loc[d, j, i] = blend(p_loc.at[d, j], f_o.at[side], wa, wb, i)
        send(d, j, onward[:2])
        return wa, wb

    def relay_last(copies, side, d, j, onward, scales):
        wait_recv(copies[2:])
        for i in range(part, half):
            p_loc[d, j, i] = blend(p_loc.at[d, j], f_o.at[side], *scales, i)
        start(onward[2:])

    def finish(ready, side, j, lo, hi, scales=None):
        wait_recv(ready)
        if scales is None:
            wa, wb, st = weights(s_loc[OWN, j], unpacked(fin_s[side, j]))
            scales = (wa, wb, 1.0 / st)
        wa, wb, inv = scales
        for i in range(lo, hi):
            o = blend(p_loc.at[OWN, j], fin_o.at[side, j], wa, wb, i) * inv[:, half + i:half + i + 1]
            att[j * tokens:(j + 1) * tokens, i * hd:(i + 1) * hd] = o.astype(BF)
        return scales

    ROWS = 16
    n_col = dim // OUT_COL

    def normalise(squares, gain):
        inv = lax.rsqrt(jnp.sum(squares, axis=1, keepdims=True) * (1.0 / dim) + NORM_EPS)
        for r in range(0, rows, ROWS):
            h[r:r + ROWS, :] = (x[r:r + ROWS, :].astype(F32) * inv[r:r + ROWS] * gain).astype(BF)

    def square_tiles(v):
        v = v * v
        return sum(v[:, c:c + 128] for c in range(0, v.shape[1], 128))

    def gain_row(ref, l):
        g = ref[0:1, :].astype(F32)
        for n in range(1, layers):
            g = jnp.where(l == n, ref[n:n + 1, :].astype(F32), g)
        return g

    def norm_only(gain):
        normalise(square_tiles(x[...].astype(F32)), gain)

    def add_norm(which, gain):
        squares = jnp.zeros((rows, 128), F32)
        for n in range(n_col):
            px_copy(which, n).wait()
            for c in range(OUT_COL // hd):
                cols = slice(n * OUT_COL + c * hd, n * OUT_COL + (c + 1) * hd)
                total = jnp.concatenate([p_send[n, j, c] + px_recv[which, n, j, c] for j in range(CORES)], axis=0)
                xv = (x[:, cols].astype(F32) + total).astype(BF)
                x[:, cols] = xv
                xv = xv.astype(F32)
                squares = squares + xv * xv
        normalise(squares, gain)

    def dot(a, b):
        return jnp.dot(a, b, preferred_element_type=F32)

    def wait_qkv(l, lo, hi):
        for t in range(lo, hi):
            for sub in range(2):
                qkv_copy(l, t, (wq, wk, wv)[t // 2], sub).wait()

    def qkv_pair(l, t):
        hv = h[...]
        for sub in range(2):
            res = dot(hv, ring[2 * t + sub])
            for e in range(COL // hd):
                v = res[:, e * hd:(e + 1) * hd]
                if t < 4:
                    v = v * cos[...] + pltpu.roll(v, hd // 2, axis=1) * sin[...]
                v = v.astype(BF)
                i = (t % 2) * part + sub * (COL // hd) + e
                for j in range(CORES):
                    vj = v[j * tokens:(j + 1) * tokens]
                    if t < 2:
                        q[chip, core, j, i] = vj
                    elif t < 4:
                        k_new[i, j] = vj
                    else:
                        v_new[i, j] = vj
    barrier = pltpu.get_barrier_semaphore()
    for dev in (partner, left, right):
        pl.semaphore_signal(barrier, inc=1, device_id={"pool": dev}, device_id_type=MESH)
    for t in range(PAIRS):
        start_qkv(0, t)
    start_pages(0)
    s_loc[...] = jnp.zeros_like(s_loc)
    s_send[...] = jnp.zeros_like(s_send)
    n_s[...] = jnp.zeros_like(n_s)
    own_rows = pl.ds(pl.multiple_of(core * tokens, tokens), tokens)
    x[own_rows, :] = hid[0]
    pl.semaphore_wait(barrier, 3)
    x_copy = remote(hid.at[0], x.at[own_rows], x_sem, partner)
    x_copy.start()
    raw[...] = jnp.zeros_like(raw)
    x_copy.wait()
    norm_only(gain_row(gain_a, 0))

    def layer(l, carry):
        wait_qkv(l, 0, 2)
        for t in range(2):
            qkv_pair(l, t)
        for n in range(2):
            q_right(n).start()
            q_left(n).start()
        for n in range(2):
            q_part(n).start()
        wait_qkv(l, 2, 6)
        for t in range(2, 6):
            qkv_pair(l, t)

        @pl.when(l == 0)
        def _():
            turn_pages(0, 0, n_pages)
        attend_pages(own_unit, core, p_loc, s_loc)
        attend_new()
        q_right(0).wait_recv()
        q_right(2).start()
        q_part(2).start()
        q_left(0).wait_recv()
        q_left(2).start()
        q_part(5).start()
        attend_pages(near_first, core, p_loc, s_loc)
        q_part(2).wait_recv()
        q_part(5).wait_recv()
        attend_pages(near_first, other, p_send, s_send)
        start(o_part(LEFT, 0))
        start(o_part(RIGHT, 1))
        q_right(1).wait_recv()
        q_part(3).start()
        q_left(1).wait_recv()
        q_part(4).start()
        attend_pages(near_last, core, p_loc, s_loc)
        merge_pair(LEFT, 0)
        send(LEFT, 0, o_left(0))
        merge_pair(RIGHT, 1)
        send(RIGHT, 1, o_right(0))
        for n in range(n_col):
            wo_copy(l, n).start()
        for t in range(PAIRS):
            for sub in range(2):
                gu_copy(l, t, sub).start()
        q_right(2).wait_recv()
        q_part(6).start()
        q_left(2).wait_recv()
        q_part(7).start()
        attend_pages(far_unit, core, p_loc, s_loc)
        q_part(6).wait_recv()
        q_part(7).wait_recv()
        attend_pages(far_unit, other, p_send, s_send)
        start(o_part(FAR, 0))
        start(o_part(FAR, 1))
        q_part(3).wait_recv()
        q_part(4).wait_recv()
        attend_pages(near_last, other, p_send, s_send)
        start(o_part(LEFT, 1))
        start(o_part(RIGHT, 0))
        merge_pair(FAR, 0)
        send(FAR, 0, o_right(1))
        merge_pair(FAR, 1)
        send(FAR, 1, o_left(1))
        q_part(0).wait_recv()
        q_part(1).wait_recv()
        attend_pages(own_unit, other, p_send, s_send)
        start(o_part(OWN, 0))
        start(o_part(OWN, 1))

        @pl.when(l + 1 < layers)
        def _():
            start_pages(l + 1)
        merge_pair(RIGHT, 0)
        merge_pair(LEFT, 1)
        for n in range(8):
            q_part(n).wait_send()
        for n in range(3):
            q_right(n).wait_send()
            q_left(n).wait_send()
        for j in range(CORES):
            merge_pair(OWN, j)
            merge(p_loc.at[OWN, j], s_loc.at[OWN, j], n_o.at[j], n_s[j])

        @pl.when(l + 1 < layers)
        def _():
            turn_pages(l + 1, 0, n_pages // 2)
        from_left = relay_first(o_right(1), 0, RIGHT, 0, o_right(2))
        from_right = relay_first(o_left(1), 1, LEFT, 1, o_left(2))
        relay_last(o_right(1), 0, RIGHT, 0, o_right(2), from_left)
        relay_last(o_left(1), 1, LEFT, 1, o_left(2), from_right)
        for n in range(dim // COL):
            wd_copy(l, n).start()
        wait_recv(o_right(0))
        merge(p_loc.at[OWN, 1], s_loc.at[OWN, 1], fin_o.at[0, 1], unpacked(fin_s[0, 1]))
        wait_recv(o_left(0))
        merge(p_loc.at[OWN, 0], s_loc.at[OWN, 0], fin_o.at[1, 0], unpacked(fin_s[1, 0]))

        @pl.when(l + 1 < layers)
        def _():
            turn_pages(l + 1, n_pages // 2, n_pages)
        first = finish(o_right(2)[:2], 0, 0, 0, part)
        second = finish(o_left(2)[:2], 1, 1, 0, part)
        finish(o_right(2)[2:], 0, 0, part, half, first)
        finish(o_left(2)[2:], 1, 1, part, half, second)
        for n in range(3):
            wait_send(o_right(n))
            wait_send(o_left(n))
        for d in range(4):
            for j in range(CORES):
                wait_send(o_part(d, j))

        for n in range(n_col):
            wo_copy(l, n).wait()
        for n in range(n_col):
            put_partial(n, 0, dot(att[...], wo_buf[n]))
            px_copy(0, n).start()
        add_norm(0, gain_row(gain_m, l))

        def gate_block(j):
            gate, upper = raw[0], raw[1]
            val = gate / (1.0 + jnp.exp(-gate)) * upper
            if j * COL < overlap:
                col = lax.broadcasted_iota(jnp.int32, (rows, COL), 1) + j * COL
                val = jnp.where(col >= core * overlap, val, 0.0)
            inner[:, j * COL:(j + 1) * COL] = val.astype(BF)

        for j in range(ff_chunks):
            if j % GATE_WAIT == 0:
                for jj in range(j, min(j + GATE_WAIT, ff_chunks)):
                    for sub in range(2):
                        gu_copy(l, jj, sub).wait()
            sp = j % PAIRS
            hv = h[...]
            gate = dot(hv, ring[2 * sp])
            upper = dot(hv, ring[2 * sp + 1])
            if j > 0:
                gate_block(j - 1)
            raw[0] = gate
            raw[1] = upper
            if j + PAIRS < ff_chunks:
                for sub in range(2):
                    gu_copy(l, j + PAIRS, sub).start()
            else:
                @pl.when(l + 1 < layers)
                def _(sp=sp):
                    for sub in range(2):
                        qkv_copy(l + 1, sp, (wq, wk, wv)[sp // 2], sub).start()
        gate_block(ff_chunks - 1)

        for n in range(dim // COL):
            wd_copy(l, n).wait()
        iv = inner[...]
        for n in range(n_col):
            for sub in range(OUT_COL // COL):
                put_partial(n, sub * (COL // hd), dot(iv, wd_buf[2 * n + sub]))
            px_copy(1, n).start()
        add_norm(1, gain_row(gain_a, lax.rem(l + 1, layers)))
        return carry
    lax.fori_loop(0, layers, layer, 0)
    out[0] = x[own_rows, :]


def solution(mesh):
    group = mesh.shape["pool"]

    def local_program(kv, idx, hid, attn_norm, w_query, w_key, w_value, w_out, mlp_norm, w_gate, w_up, w_down):
        layers, n_pages, _, page_len, heads, hd = kv.shape
        slots = idx.shape[2]
        _, tokens, dim = hid.shape
        ff = w_gate.shape[2]
        half, rows = heads // CORES, CORES * tokens
        ff_cols = -(-ff // (CORES * COL)) * COL
        cosine, sine = rope_tables(group * slots * page_len, tokens, hd)
        cos2 = jnp.asarray(np.tile(cosine, (CORES, 1)))
        sin2 = jnp.asarray(np.tile(sine, (CORES, 1)))
        cfg = (layers, tokens, dim, heads, hd, ff, n_pages, slots)
        vmem = pl.BlockSpec(memory_space=pltpu.VMEM)
        hbm = pl.BlockSpec(memory_space=pl.ANY)
        smem = pl.BlockSpec(memory_space=pltpu.SMEM)
        dma = pltpu.SemaphoreType.DMA
        o_block = (half, tokens, hd)
        s_block, t_block = (tokens, 128), (8, 128)
        n_out = dim // OUT_COL
        scratch = [
            pltpu.VMEM((rows, dim), BF), pltpu.VMEM((rows, dim), BF), pltpu.VMEM((rows, half * hd), BF), pltpu.VMEM((rows, ff_cols), BF),
            pltpu.VMEM((CHIPS, CORES, CORES, half, tokens, hd), BF),
            pltpu.VMEM((half, CORES, tokens, hd), BF), pltpu.VMEM((half, CORES, tokens, hd), BF),
            pltpu.VMEM((n_pages, 2, page_len * heads, hd), BF),
            pltpu.VMEM((TURN, 2, heads * PITCH, hd), F32),
            pltpu.VMEM((4, CORES) + o_block, F32), pltpu.VMEM((4, CORES) + o_block, F32), pltpu.VMEM((4, CORES) + o_block, F32),
            pltpu.VMEM((4, CORES) + s_block, F32), pltpu.VMEM((4, CORES) + s_block, F32), pltpu.VMEM((4, CORES) + s_block, F32),
            pltpu.VMEM((4, CORES) + t_block, F32),
            pltpu.VMEM((CORES,) + o_block, F32), pltpu.VMEM((CORES,) + s_block, F32),
            pltpu.VMEM((2,) + o_block, F32), pltpu.VMEM((2,) + t_block, F32),
            pltpu.VMEM((2, CORES) + o_block, F32), pltpu.VMEM((2, CORES) + t_block, F32),
            pltpu.VMEM((2, n_out, CORES, OUT_COL // hd, tokens, hd), F32), pltpu.VMEM((2, rows, COL), F32),
            pltpu.VMEM((2 * PAIRS, dim, COL), BF), pltpu.VMEM((n_out, half * hd, OUT_COL), BF), pltpu.VMEM((dim // COL, ff_cols, COL), BF),
            dma((2 * PAIRS,)), dma((n_out,)), dma((dim // COL,)), dma((n_pages,)),
            dma((2,)), dma((8, 2)), dma((3, 2)), dma((3, 2)), dma((4, CORES, 2, 2)), dma((3, 3, 2)), dma((3, 3, 2)), dma((2, n_out, 2)),
        ]
        result = pl.pallas_call(
            functools.partial(kernel, cfg),
            out_shape=jax.ShapeDtypeStruct((1, tokens, dim), BF),
            in_specs=[smem] + [vmem] * 5 + [hbm] * 8,
            out_specs=vmem,
            scratch_shapes=scratch,
            compiler_params=pltpu.CompilerParams(collective_id=0, has_side_effects=True, vmem_limit_bytes=67043328),
            name="decoder",
        )(idx, hid, cos2, sin2, attn_norm, mlp_norm,
          kv.reshape(layers, n_pages, 2, page_len * heads, hd), w_query, w_key, w_value, w_out, w_gate, w_up, w_down)
        return result

    data_specs = (P(None, ("rep", "pool")), P(None, ("rep", "pool"), None), P(("rep", "pool")))
    return jax.shard_map(local_program, mesh=mesh, in_specs=data_specs + (P(),) * 9, out_specs=P(("rep", "pool")), check_vma=False)
```
